128 devices in a mesh: filt: 4 (over x), dom: 32 (over y, z, core).
Axes of the slice: x: 4, y: 4, z: 4, core: 2. Of those that a mesh axis runs over, the one named last changes fastest.
Arguments:
- log_weights: float32 [2097152], P(('filt', 'dom')), parts along dimension 0, may hold values from -20 to 250, as said below
- bins: int32 [2097152], P(('filt', 'dom')), parts along dimension 0, may hold values from 0 to 4095
- states: bfloat16 [128, 2097152], P(None, ('filt', 'dom')), parts along dimension 1, may hold values from -6 to 6
Outputs:
- cumulative: float32 [16384], P(('filt', 'dom')), parts along dimension 0
- bin_means: float32 [128, 16384], P(None, ('filt', 'dom')), parts along dimension 1
- particle_weights: float32 [2097152], P(('filt', 'dom')), parts along dimension 0
The draws below stay inside these ranges and needn't reach their ends.
There are 4 independent parts, one for each index of `filt`. The reference program is written for one: setup_inputs(seed, part) draws one part's arguments, and reference() takes and returns one part's arrays. A program takes and returns all parts, laid end to end along the dimension named above; each array names one. Nothing has to cross between parts.
Inputs may be any that keep to these rules, and one draw needn't show every extreme that they name: `log_weights`: finite log-weights.
All inputs are finite; a program needn't handle non-finite values.
Results may differ from the reference program's by a relative error of at most 0.00051.
Values sent between devices are 32-bit elements; how exact they have to be, the bound alone decides.
A program may use at most 64 MiB of HBM per device.

```python
import math
import jax
import jax.numpy as jnp
import numpy as np
from jax import lax

BINS = 4096
STATE = 128
P_DEV = 16384
PARTICLES = 524288
N_DOM = 32


def draw_log_weights(key, part):
    key_offset, key_noise = jax.random.split(jax.random.fold_in(key, 7))
    groups = PARTICLES // P_DEV
    offsets = jax.random.uniform(key_offset, (groups,), jnp.float32, -3.0, 3.0)
    noise = jnp.clip(1.5 * jax.random.normal(key_noise, (groups, P_DEV), jnp.float32), -8.0, 8.0)
    return (offsets[:, None] + noise).reshape(PARTICLES).astype(jnp.float32)


def set_ends(entries, stream_key, least, top_value):
    dims = entries.shape
    spot = [jax.random.randint(jax.random.fold_in(stream_key, axis), (), 0, dims[axis]) for axis in range(len(dims))]
    entries = entries.at[tuple(spot)].set(least)
    longest = dims.index(max(dims))
    spot[longest] = (spot[longest] + 1) % dims[longest]
    return entries.at[tuple(spot)].set(top_value)


def level_of(rng, dims, cuts, smallest, largest):
    gain = 1.0
    for axis_at, blocks in cuts:
        heights = jax.random.uniform(jax.random.fold_in(jax.random.fold_in(rng, 6), axis_at), (blocks,), jnp.float32, smallest / len(cuts), largest / len(cuts))
        gain = gain * jnp.repeat(jnp.exp(heights), dims[axis_at] // blocks).reshape((-1,) + (1,) * (len(dims) - 1 - axis_at))
    return gain


def rank_bounds(count, slope):
    weights = [(1 << 20) // math.isqrt(grade ** slope) + 1 for grade in range(1, count + 1)]
    scale = 1 + sum(weights) // (1 << 30)
    return np.cumsum(np.array([max(1, weight // scale) for weight in weights]))


def ranked(key, extent, amount, lean):
    table = rank_bounds(amount, lean)
    pick = jax.random.randint(jax.random.fold_in(key, 1), extent, 0, int(table[amount - 1]))
    rank = jnp.searchsorted(jnp.asarray(table, jnp.int32), pick, side="right")
    return jax.random.permutation(jax.random.fold_in(key, 2), amount)[rank].astype(jnp.int32)


def scatter_about(stream_key, dims, scale, limit, pieces=(), held_as=jnp.bfloat16):
    level = level_of(stream_key, dims, pieces, -0.22, 0.18) if pieces else 1.0
    entries = jax.random.normal(stream_key, dims, jnp.float32) * scale * level
    return jnp.minimum(jnp.maximum(entries, -limit), limit).astype(held_as)


def setup_inputs(seed: int = 0, part: int = 0) -> dict:
    key_of = jax.random.split(jax.random.key(seed), 4)
    part_splits = jax.random.split(jax.random.fold_in(key_of[3], part), 4)
    log_weights = draw_log_weights(jax.random.fold_in(jax.random.fold_in(key_of[3], part), 71), part)
    bins = set_ends(ranked(part_splits[1], (PARTICLES,), BINS, 2), jax.random.fold_in(part_splits[1], 3), 0, BINS - 1).astype(jnp.int32)
    states = scatter_about(part_splits[2], (STATE, PARTICLES), 1.0, 6.0, ((1, 32),))
    return dict(log_weights=log_weights, bins=bins, states=states)


floor_value = -1.0e4


def group_pairs(group_weights, group_bins, group_states):
    width = min(P_DEV, 1024)
    blocks = P_DEV // width
    labels = lax.iota(jnp.int32, BINS)

    def top_step(index, carry):
        start = (index * width).astype(jnp.int32)
        row_weights = lax.dynamic_slice_in_dim(group_weights, start, width)
        row_bins = lax.dynamic_slice_in_dim(group_bins, start, width)
        member = row_bins[:, None] == labels[None, :]
        return jnp.maximum(carry, jnp.max(jnp.where(member, row_weights[:, None], floor_value), axis=0))

    bin_top = lax.fori_loop(0, blocks, top_step, jnp.full((BINS,), floor_value, jnp.float32))

    def sum_step(index, carry):
        totals, sums = carry
        start = (index * width).astype(jnp.int32)
        row_weights = lax.dynamic_slice_in_dim(group_weights, start, width)
        row_bins = lax.dynamic_slice_in_dim(group_bins, start, width)
        row_states = lax.dynamic_slice_in_dim(group_states, start, width, 1).astype(jnp.float32)
        member = row_bins[:, None] == labels[None, :]
        own_top = jnp.sum(jnp.where(member, bin_top[None, :], jnp.float32(0.0)), axis=1)
        scaled = jnp.exp(row_weights - own_top).astype(jnp.bfloat16).astype(jnp.float32)
        spread = jnp.where(member, scaled[:, None], jnp.float32(0.0))
        totals = totals + jnp.sum(spread, axis=0)
        sums = sums + jnp.dot(row_states, spread, precision=lax.Precision.HIGHEST, preferred_element_type=jnp.float32)
        return totals, sums

    start_pair = (jnp.zeros((BINS,), jnp.float32), jnp.zeros((STATE, BINS), jnp.float32))
    totals, sums = lax.fori_loop(0, blocks, sum_step, start_pair)
    return bin_top, totals, sums


def reference(log_weights, bins, states):
    def one_group(group):
        start = (group * P_DEV).astype(jnp.int32)
        return group_pairs(lax.dynamic_slice_in_dim(log_weights, start, P_DEV),
                           lax.dynamic_slice_in_dim(bins, start, P_DEV),
                           lax.dynamic_slice_in_dim(states, start, P_DEV, 1))

    local_top, local_mass, local_sums = lax.map(one_group, jnp.arange(N_DOM, dtype=jnp.int32))
    bin_top = jnp.max(local_top, axis=0)
    factor = jnp.exp(local_top - bin_top[None, :])
    bin_mass = jnp.sum(local_mass * factor, axis=0)
    bin_sums = jnp.sum(local_sums * factor[:, None, :], axis=0)
    top = jnp.max(bin_top)
    share = bin_mass * jnp.exp(bin_top - top)
    total = jnp.sum(share)
    cumulative = jnp.cumsum(share) / total
    bin_means = bin_sums / jnp.maximum(bin_mass, 1.0)[None, :]
    particle_weights = (P_DEV * N_DOM) * jnp.exp(log_weights - top) / total
    return cumulative, bin_means, particle_weights
```

```python
import functools
import jax
import jax.numpy as jnp
from jax import lax
from jax.experimental import pallas as pl
from jax.experimental.pallas import tpu as pltpu
from jax.sharding import PartitionSpec as P

BINS = 4096
FLOOR = -10000.0
COUNT = 16384
STATE = 128
HALVES = 2
ROWS = STATE // HALVES
CHUNKS = COUNT // 256


def shuffle(x, sub, lane):
    if sub:
        x = jnp.take_along_axis(x, lax.broadcasted_iota(jnp.int32, (8, 128), 0) ^ sub, axis=0,
                                mode="promise_in_bounds")
    if lane:
        x = jnp.take_along_axis(x, lax.broadcasted_iota(jnp.int32, (8, 128), 1) ^ lane, axis=1,
                                mode="promise_in_bounds")
    return x


def is_high(bit):
    if bit < 7:
        return ((lax.broadcasted_iota(jnp.int32, (8, 128), 0) >> (bit - 4)) & 1) == 1
    return ((lax.broadcasted_iota(jnp.int32, (8, 128), 1) >> (bit - 7)) & 1) == 1


def network():
    steps = []
    for k in range(1, 15):
        steps.append((1 << k) - 1)
        for j in range(k - 2, -1, -1):
            steps.append(1 << j)
    return steps


def swap_step(keys, vals, flip, mark_ref, slot):
    top_bit = flip.bit_length() - 1
    vec, sub, lane = flip & 15, (flip >> 4) & 7, flip >> 7
    keys, vals = list(keys), list(vals)
    if not sub and not lane:
        for r in range(16):
            if (r >> top_bit) & 1:
                continue
            q = r ^ vec
            swap = keys[r] > keys[q]
            mark_ref[slot] = swap.astype(jnp.int32)
            slot += 1
            keys[r], keys[q] = jnp.where(swap, keys[q], keys[r]), jnp.where(swap, keys[r], keys[q])
            vals[r], vals[q] = jnp.where(swap, vals[q], vals[r]), jnp.where(swap, vals[r], vals[q])
        return keys, vals, slot
    high = is_high(top_bit)
    other_keys = [shuffle(x, sub, lane) for x in keys]
    other_vals = [shuffle(x, sub, lane) for x in vals]
    out_keys, out_vals = [], []
    for r in range(16):
        q = r ^ vec
        take = (keys[r] > other_keys[q]) ^ high
        mark_ref[slot] = take.astype(jnp.int32)
        slot += 1
        out_keys.append(jnp.where(take, other_keys[q], keys[r]))
        out_vals.append(jnp.where(take, other_vals[q], vals[r]))
    return out_keys, out_vals, slot


def undo_step(vals, flip, mark_ref, slot):
    top_bit = flip.bit_length() - 1
    vec, sub, lane = flip & 15, (flip >> 4) & 7, flip >> 7
    vals = list(vals)
    if not sub and not lane:
        slot -= 8
        at = slot
        for r in range(16):
            if (r >> top_bit) & 1:
                continue
            q = r ^ vec
            swap = mark_ref[at] != 0
            at += 1
            vals[r], vals[q] = jnp.where(swap, vals[q], vals[r]), jnp.where(swap, vals[r], vals[q])
        return vals, slot
    slot -= 16
    others = [shuffle(x, sub, lane) for x in vals]
    return [jnp.where(mark_ref[slot + r] != 0, others[r ^ vec], vals[r]) for r in range(16)], slot


def rotate(x, by, axis):
    size = x.shape[axis]
    at = (lax.broadcasted_iota(jnp.int32, (8, 128), axis) + by) & (size - 1)
    return jnp.take_along_axis(x, at, axis=axis, mode="promise_in_bounds")


def shifted(vecs, by):
    step = abs(by)
    sign = 1 if by > 0 else -1
    if step >= 128:
        return [rotate(x, by // 128, 1) for x in vecs]
    sublane = lax.broadcasted_iota(jnp.int32, (8, 128), 0)

    def carry_sub(x, m):
        moved = rotate(x, m, 0)
        crossed = rotate(moved, sign, 1)
        inside = (sublane + m < 8) if m > 0 else (sublane + m >= 0)
        return jnp.where(inside, moved, crossed)

    if step >= 16:
        return [carry_sub(x, by // 16) for x in vecs]
    out = []
    for r in range(16):
        q = r + by
        out.append(vecs[q] if 0 <= q < 16 else carry_sub(vecs[q % 16], sign))
    return out


def segment_tops(groups, vals):
    for sign in (1, -1):
        for level in range(14):
            by = sign * (1 << level)
            near_groups, near_vals = shifted(groups, by), shifted(vals, by)
            vals = [
                jnp.where(g == ng, jnp.maximum(v, nv), v)
                for g, ng, v, nv in zip(groups, near_groups, vals, near_vals)
            ]
    return vals


def own_tops(bins_ref, weights_ref, mark_ref):
    lane = lax.broadcasted_iota(jnp.int32, (8, 128), 1)
    sublane = lax.broadcasted_iota(jnp.int32, (8, 128), 0)
    keys, vals = [], []
    for r in range(16):
        rows = pl.ds(8 * r, 8)
        keys.append(bins_ref[rows, :] * COUNT + (lane * 128 + sublane * 16 + r))
        vals.append(weights_ref[rows, :])
    slot = 0
    for flip in network():
        keys, vals, slot = swap_step(keys, vals, flip, mark_ref, slot)
    groups = [k >> 14 for k in keys]
    vals = segment_tops(groups, vals)
    for flip in reversed(network()):
        vals, slot = undo_step(vals, flip, mark_ref, slot)
    return vals


MARKS = sum(8 if flip < 16 else 16 for flip in network())


def rows_of(ref, chunk):
    return jnp.concatenate([ref[pl.ds(2 * chunk, 1), :], ref[pl.ds(2 * chunk + 1, 1), :]], axis=1)


def tile_of(row):
    return jnp.broadcast_to(row, (16, 256)).astype(jnp.bfloat16)


def local_kernel(bins_ref, weights_ref, states_hbm, sums_ref, mass_ref, top_ref, mark_ref,
                 states_ref, iota_ref, key0_ref, key1_ref, part_ref, scaled_ref, flag_ref, t1_ref,
                 t2_ref, t3_ref, copy_sem):
    load = pltpu.make_async_copy(states_hbm, states_ref, copy_sem)
    load.start()
    tops = own_tops(bins_ref, weights_ref, mark_ref)
    for r in range(16):
        rows = pl.ds(8 * r, 8)
        w, b, top = weights_ref[rows, :], bins_ref[rows, :], tops[r]
        flag = w == top
        scaled = jnp.where(flag, 1.0, jnp.exp(w - top))
        scaled_ref[rows, :] = scaled
        low = (b & 255).astype(jnp.float32)
        upper = (b & 256) != 0
        key0_ref[rows, :] = jnp.where(upper, -1.0, low)
        key1_ref[rows, :] = jnp.where(upper, low, -1.0)
        part_ref[rows, :] = (b >> 9).astype(jnp.float32)
        t1 = top.astype(jnp.bfloat16).astype(jnp.float32)
        t2 = (top - t1).astype(jnp.bfloat16).astype(jnp.float32)
        t3 = top - t1 - t2
        flag_ref[rows, :] = jnp.where(flag, 1.0, 0.0)
        t1_ref[rows, :] = jnp.where(flag, t1, 0.0)
        t2_ref[rows, :] = jnp.where(flag, t2, 0.0)
        t3_ref[rows, :] = jnp.where(flag, t3, 0.0)
    iota_ref[...] = lax.broadcasted_iota(jnp.int32, (256, 128), 0).astype(jnp.float32).astype(jnp.bfloat16)
    load.wait()

    def push(chunk, register):
        scaled = tile_of(rows_of(scaled_ref, chunk))
        for q, key_ref in enumerate((key0_ref, key1_ref)):
            key = tile_of(rows_of(key_ref, chunk))
            halves = []
            for side in range(2):
                lanes = slice(128 * side, 128 * side + 128)
                key_full = jnp.concatenate([key[:, lanes]] * 16, axis=0)
                scaled_full = jnp.concatenate([scaled[:, lanes]] * 16, axis=0)
                halves.append(jnp.where(iota_ref[...] == key_full, scaled_full, jnp.bfloat16(0)))
            pltpu.matmul_push_rhs(jnp.concatenate(halves, axis=1), staging_register=register,
                                  mxu_index=q, transpose=True)

    def run(*accs):
        accs = (accs[:9], accs[9:])

        def multiply(chunk, register, half):
            part = tile_of(rows_of(part_ref, chunk))
            cols = pl.ds(pl.multiple_of(chunk * 256, 256), 256)
            block = states_ref[pl.ds(half * ROWS, ROWS), cols]
            for p in range(8):
                mask = jnp.where(part == p, jnp.bfloat16(1), jnp.bfloat16(0))
                lhs = block * jnp.concatenate([mask] * (ROWS // 16), axis=0)
                for q in range(2):
                    pltpu.matmul_acc_lhs(accs[q][p], lhs,
                                         load_staged_rhs=register if p == 0 else None)
            if half == 0:
                row = lax.broadcasted_iota(jnp.int32, (16, 256), 0)
                lower = row < 8
                mine = (row & 7).astype(jnp.float32) == jnp.broadcast_to(rows_of(part_ref, chunk), (16, 256))
                flag, t1, t2, t3 = (
                    jnp.broadcast_to(rows_of(ref, chunk), (16, 256))
                    for ref in (flag_ref, t1_ref, t2_ref, t3_ref)
                )
                groups = (jnp.where(lower, 1.0, flag), jnp.where(lower, t1, t2), jnp.where(lower, t3, 0.0))
                lhs = jnp.concatenate(
                    [jnp.where(mine, g, 0.0).astype(jnp.bfloat16) for g in groups], axis=0)
                for q in range(2):
                    pltpu.matmul_acc_lhs(accs[q][8], lhs)

        for q in range(2):
            for a in accs[q]:
                pltpu.matmul_pop(a)
        push(0, 0)
        for half in range(HALVES):
            @pl.loop(0, CHUNKS, step=2)
            def _(chunk):
                multiply(chunk, 0, half)
                push(chunk + 1, 1)
                multiply(chunk + 1, 1, half)
                push((chunk + 2) & (CHUNKS - 1), 0)

            for p in range(8):
                for q in range(2):
                    sums_ref[ROWS * half:ROWS * half + ROWS, 512 * p + 256 * q:512 * p + 256 * q + 256] = (
                        pltpu.matmul_pop(accs[q][p]))
            if half == 0:
                for q in range(2):
                    extra = pltpu.matmul_pop(accs[q][8])
                    cols = slice(256 * q, 256 * q + 256)
                    mass_ref[:, cols] = extra[0:8]
                    hits = extra[8:16]
                    each = jnp.maximum(hits, 1.0)
                    t1, t2, t3 = (
                        (extra[8 * i:8 * i + 8] / each).astype(jnp.bfloat16).astype(jnp.float32)
                        for i in (2, 3, 4)
                    )
                    top_ref[:, cols] = jnp.where(hits > 0.0, (t1 + t2) + t3, FLOOR)
        for q in range(2):
            pltpu.matmul_acc_lhs(accs[q][8], jnp.zeros((48, 256), jnp.bfloat16), load_staged_rhs=0)
            pltpu.matmul_pop(accs[q][8])

    specs = []
    for q in range(2):
        specs += [pltpu.ACC(q)((ROWS, 256), jnp.float32)] * 8 + [pltpu.ACC(q)((48, 256), jnp.float32)]
    pl.run_scoped(run, *specs)


def local_sums(log_weights, bins, states):
    vmem = pl.BlockSpec(memory_space=pltpu.VMEM)
    table = pltpu.VMEM((128, 128), jnp.float32)
    return pl.pallas_call(
        local_kernel,
        out_shape=(
            jax.ShapeDtypeStruct((STATE, BINS), jnp.float32),
            jax.ShapeDtypeStruct((8, 512), jnp.float32),
            jax.ShapeDtypeStruct((8, 512), jnp.float32),
        ),
        in_specs=[vmem, vmem, pl.BlockSpec(memory_space=pl.ANY)],
        out_specs=(vmem, vmem, vmem),
        scratch_shapes=[
            pltpu.VMEM((MARKS, 8, 128), jnp.int32),
            pltpu.VMEM((STATE, COUNT), jnp.bfloat16),
            pltpu.VMEM((256, 128), jnp.bfloat16),
        ] + [table] * 8 + [pltpu.SemaphoreType.DMA],
        compiler_params=pltpu.CompilerParams(vmem_limit_bytes=40 * 1024 * 1024),
        name="local_sums",
    )(bins.reshape(128, 128), log_weights.reshape(128, 128), states)


def rows_first(arrays, axis, dims):
    turned = [jnp.moveaxis(a, dim, 0) for a, dim in zip(arrays, dims)]
    both = jnp.concatenate([t.reshape(len(t), -1) for t in turned], axis=1)
    out, at, finished = (lax.all_gather(both, axis, axis=0, tiled=True), 0, [])
    for t, dim in zip(turned, dims):
        piece = out[:, at : at + t[0].size].reshape(-1, *t.shape[1:])
        finished.append(jnp.moveaxis(piece, 0, dim))
        at += t[0].size
    return tuple(finished)


def body(log_weights, bins, states):
    groups = lax.axis_size("dom")
    owned = BINS // groups
    sums, totals, bin_top = local_sums(log_weights, bins, states)
    both = jnp.stack([bin_top.reshape(BINS), totals.reshape(BINS)])
    pieces = lax.all_to_all(both, "dom", split_axis=1, concat_axis=0, tiled=True).reshape(groups, 2, owned)
    top_pieces, mass_pieces = pieces[:, 0], pieces[:, 1]
    sum_pieces = lax.all_to_all(sums, "dom", split_axis=1, concat_axis=0, tiled=True)
    sum_pieces = sum_pieces.reshape(groups, sums.shape[0], owned)
    owned_top = jnp.max(top_pieces, axis=0)
    factor = jnp.exp(top_pieces - owned_top[None, :])
    owned_mass = jnp.sum(mass_pieces * factor, axis=0)
    owned_sums = jnp.sum(sum_pieces * factor[:, None, :], axis=0)
    block_top = jnp.max(owned_top)
    block_mass = jnp.sum(owned_mass * jnp.exp(owned_top - block_top))
    all_tops, all_masses = rows_first((block_top[None], block_mass[None]), "dom", (0, 0))
    top = jnp.max(all_tops)
    scaled_masses = all_masses * jnp.exp(all_tops - top)
    total = jnp.sum(scaled_masses)
    lower = lax.iota(jnp.int32, groups) < lax.axis_index("dom")
    before = jnp.sum(jnp.where(lower, scaled_masses, jnp.float32(0.0)))
    share = owned_mass * jnp.exp(owned_top - top)
    cumulative = (before + jnp.cumsum(share)) / total
    bin_means = owned_sums / jnp.maximum(owned_mass, 1.0)[None, :]
    whole_count = log_weights.shape[0] * groups
    particle_weights = whole_count * jnp.exp(log_weights - top) / total
    return (cumulative, bin_means, particle_weights)


def solution(mesh):
    placed = (P(("filt", "dom")), P(("filt", "dom")), P(None, ("filt", "dom")))
    return jax.shard_map(
        body,
        mesh=mesh,
        in_specs=placed,
        out_specs=(P(("filt", "dom")), P(None, ("filt", "dom")), P(("filt", "dom"))),
        check_vma=False,
    )
```

```python
import functools
import jax
import jax.numpy as jnp
from jax import lax
from jax.experimental import pallas as pl
from jax.experimental.pallas import tpu as pltpu
from jax.sharding import PartitionSpec as P

BINS = 4096
FLOOR = -10000.0
COUNT = 16384
STATE = 128
HALVES = 2
ROWS = STATE // HALVES
CHUNKS = COUNT // 256


def shuffle(x, sub, lane):
    if sub:
        x = jnp.take_along_axis(x, lax.broadcasted_iota(jnp.int32, (8, 128), 0) ^ sub, axis=0,
                                mode="promise_in_bounds")
    if lane:
        x = jnp.take_along_axis(x, lax.broadcasted_iota(jnp.int32, (8, 128), 1) ^ lane, axis=1,
                                mode="promise_in_bounds")
    return x


def is_high(bit):
    if bit < 7:
        return ((lax.broadcasted_iota(jnp.int32, (8, 128), 0) >> (bit - 4)) & 1) == 1
    return ((lax.broadcasted_iota(jnp.int32, (8, 128), 1) >> (bit - 7)) & 1) == 1


def network():
    steps = []
    for k in range(1, 15):
        steps.append((1 << k) - 1)
        for j in range(k - 2, -1, -1):
            steps.append(1 << j)
    return steps


def swap_step(keys, vals, flip, mark_ref, slot):
    top_bit = flip.bit_length() - 1
    vec, sub, lane = flip & 15, (flip >> 4) & 7, flip >> 7
    keys, vals = list(keys), list(vals)
    if not sub and not lane:
        for r in range(16):
            if (r >> top_bit) & 1:
                continue
            q = r ^ vec
            swap = keys[r] > keys[q]
            mark_ref[slot] = swap.astype(jnp.int32)
            slot += 1
            keys[r], keys[q] = jnp.where(swap, keys[q], keys[r]), jnp.where(swap, keys[r], keys[q])
            vals[r], vals[q] = jnp.where(swap, vals[q], vals[r]), jnp.where(swap, vals[r], vals[q])
        return keys, vals, slot
    high = is_high(top_bit)
    other_keys = [shuffle(x, sub, lane) for x in keys]
    other_vals = [shuffle(x, sub, lane) for x in vals]
    out_keys, out_vals = [], []
    for r in range(16):
        q = r ^ vec
        take = (keys[r] > other_keys[q]) ^ high
        mark_ref[slot] = take.astype(jnp.int32)
        slot += 1
        out_keys.append(jnp.where(take, other_keys[q], keys[r]))
        out_vals.append(jnp.where(take, other_vals[q], vals[r]))
    return out_keys, out_vals, slot


def undo_step(vals, flip, mark_ref, slot):
    top_bit = flip.bit_length() - 1
    vec, sub, lane = flip & 15, (flip >> 4) & 7, flip >> 7
    vals = list(vals)
    if not sub and not lane:
        slot -= 8
        at = slot
        for r in range(16):
            if (r >> top_bit) & 1:
                continue
            q = r ^ vec
            swap = mark_ref[at] != 0
            at += 1
            vals[r], vals[q] = jnp.where(swap, vals[q], vals[r]), jnp.where(swap, vals[r], vals[q])
        return vals, slot
    slot -= 16
    others = [shuffle(x, sub, lane) for x in vals]
    return [jnp.where(mark_ref[slot + r] != 0, others[r ^ vec], vals[r]) for r in range(16)], slot


def rotate(x, by, axis):
    size = x.shape[axis]
    at = (lax.broadcasted_iota(jnp.int32, (8, 128), axis) + by) & (size - 1)
    return jnp.take_along_axis(x, at, axis=axis, mode="promise_in_bounds")


def shifted(vecs, by):
    step = abs(by)
    sign = 1 if by > 0 else -1
    if step >= 128:
        return [rotate(x, by // 128, 1) for x in vecs]
    sublane = lax.broadcasted_iota(jnp.int32, (8, 128), 0)

    def carry_sub(x, m):
        moved = rotate(x, m, 0)
        crossed = rotate(moved, sign, 1)
        inside = (sublane + m < 8) if m > 0 else (sublane + m >= 0)
        return jnp.where(inside, moved, crossed)

    if step >= 16:
        return [carry_sub(x, by // 16) for x in vecs]
    out = []
    for r in range(16):
        q = r + by
        out.append(vecs[q] if 0 <= q < 16 else carry_sub(vecs[q % 16], sign))
    return out


def segment_tops(groups, vals):
    for sign in (1, -1):
        for level in range(14):
            by = sign * (1 << level)
            near_groups, near_vals = shifted(groups, by), shifted(vals, by)
            vals = [
                jnp.where(g == ng, jnp.maximum(v, nv), v)
                for g, ng, v, nv in zip(groups, near_groups, vals, near_vals)
            ]
    return vals


def own_tops(bins_ref, weights_ref, mark_ref):
    lane = lax.broadcasted_iota(jnp.int32, (8, 128), 1)
    sublane = lax.broadcasted_iota(jnp.int32, (8, 128), 0)
    keys, vals = [], []
    for r in range(16):
        rows = pl.ds(8 * r, 8)
        keys.append(bins_ref[rows, :] * COUNT + (lane * 128 + sublane * 16 + r))
        vals.append(weights_ref[rows, :])
    slot = 0
    for flip in network():
        keys, vals, slot = swap_step(keys, vals, flip, mark_ref, slot)
    groups = [k >> 14 for k in keys]
    vals = segment_tops(groups, vals)
    for flip in reversed(network()):
        vals, slot = undo_step(vals, flip, mark_ref, slot)
    return vals


MARKS = sum(8 if flip < 16 else 16 for flip in network())


def rows_of(ref, chunk):
    return jnp.concatenate([ref[pl.ds(2 * chunk, 1), :], ref[pl.ds(2 * chunk + 1, 1), :]], axis=1)


def tile_of(row):
    return jnp.broadcast_to(row, (16, 256)).astype(jnp.bfloat16)


def local_kernel(bins_ref, weights_ref, states_hbm, sums_ref, tab_ref, mark_ref,
                 states_ref, iota_ref, key0_ref, key1_ref, part_ref, scaled_ref, flag_ref, t1_ref,
                 t2_ref, t3_ref, copy_sem):
    load = pltpu.make_async_copy(states_hbm, states_ref, copy_sem)
    load.start()
    tops = own_tops(bins_ref, weights_ref, mark_ref)
    for r in range(16):
        rows = pl.ds(8 * r, 8)
        w, b, top = weights_ref[rows, :], bins_ref[rows, :], tops[r]
        flag = w == top
        scaled = jnp.where(flag, 1.0, jnp.exp(w - top))
        scaled_ref[rows, :] = scaled
        low = (b & 255).astype(jnp.float32)
        upper = (b & 256) != 0
        key0_ref[rows, :] = jnp.where(upper, -1.0, low)
        key1_ref[rows, :] = jnp.where(upper, low, -1.0)
        part_ref[rows, :] = (b >> 9).astype(jnp.float32)
        t1 = top.astype(jnp.bfloat16).astype(jnp.float32)
        t2 = (top - t1).astype(jnp.bfloat16).astype(jnp.float32)
        t3 = top - t1 - t2
        flag_ref[rows, :] = jnp.where(flag, 1.0, 0.0)
        t1_ref[rows, :] = jnp.where(flag, t1, 0.0)
        t2_ref[rows, :] = jnp.where(flag, t2, 0.0)
        t3_ref[rows, :] = jnp.where(flag, t3, 0.0)
    iota_ref[...] = lax.broadcasted_iota(jnp.int32, (256, 128), 0).astype(jnp.float32).astype(jnp.bfloat16)
    load.wait()

    def push(chunk, register):
        scaled = tile_of(rows_of(scaled_ref, chunk))
        for q, key_ref in enumerate((key0_ref, key1_ref)):
            key = tile_of(rows_of(key_ref, chunk))
            halves = []
            for side in range(2):
                lanes = slice(128 * side, 128 * side + 128)
                key_full = jnp.concatenate([key[:, lanes]] * 16, axis=0)
                scaled_full = jnp.concatenate([scaled[:, lanes]] * 16, axis=0)
                halves.append(jnp.where(iota_ref[...] == key_full, scaled_full, jnp.bfloat16(0)))
            pltpu.matmul_push_rhs(jnp.concatenate(halves, axis=1), staging_register=register,
                                  mxu_index=q, transpose=True)

    def run(*accs):
        accs = (accs[:9], accs[9:])

        def multiply(chunk, register, half):
            part = tile_of(rows_of(part_ref, chunk))
            cols = pl.ds(pl.multiple_of(chunk * 256, 256), 256)
            block = states_ref[pl.ds(half * ROWS, ROWS), cols]
            for p in range(8):
                mask = jnp.where(part == p, jnp.bfloat16(1), jnp.bfloat16(0))
                lhs = block * jnp.concatenate([mask] * (ROWS // 16), axis=0)
                for q in range(2):
                    pltpu.matmul_acc_lhs(accs[q][p], lhs,
                                         load_staged_rhs=register if p == 0 else None)
            if half == 0:
                row = lax.broadcasted_iota(jnp.int32, (16, 256), 0)
                lower = row < 8
                mine = (row & 7).astype(jnp.float32) == jnp.broadcast_to(rows_of(part_ref, chunk), (16, 256))
                flag, t1, t2, t3 = (
                    jnp.broadcast_to(rows_of(ref, chunk), (16, 256))
                    for ref in (flag_ref, t1_ref, t2_ref, t3_ref)
                )
                groups = (jnp.where(lower, 1.0, flag), jnp.where(lower, t1, t2), jnp.where(lower, t3, 0.0))
                lhs = jnp.concatenate(
                    [jnp.where(mine, g, 0.0).astype(jnp.bfloat16) for g in groups], axis=0)
                for q in range(2):
                    pltpu.matmul_acc_lhs(accs[q][8], lhs)

        for q in range(2):
            for a in accs[q]:
                pltpu.matmul_pop(a)
        push(0, 0)
        for half in range(HALVES):
            @pl.loop(0, CHUNKS, step=2)
            def _(chunk):
                multiply(chunk, 0, half)
                push(chunk + 1, 1)
                multiply(chunk + 1, 1, half)
                push((chunk + 2) & (CHUNKS - 1), 0)

            for p in range(8):
                for q in range(2):
                    got = pltpu.matmul_pop(accs[q][p])
                    for side in range(2):
                        sums_ref[4 * p + 2 * q + side, ROWS * half:ROWS * half + ROWS, :] = (
                            got[:, 128 * side:128 * side + 128])
            if half == 0:
                for q in range(2):
                    extra = pltpu.matmul_pop(accs[q][8])
                    hits = extra[8:16]
                    each = jnp.maximum(hits, 1.0)
                    t1, t2, t3 = (
                        (extra[8 * i:8 * i + 8] / each).astype(jnp.bfloat16).astype(jnp.float32)
                        for i in (2, 3, 4)
                    )
                    top = jnp.where(hits > 0.0, (t1 + t2) + t3, FLOOR)
                    for side in range(2):
                        lanes = slice(128 * side, 128 * side + 128)
                        tab_ref[pl.ds(2 * q + side, 8, stride=4), :] = top[:, lanes]
                        tab_ref[pl.ds(32 + 2 * q + side, 8, stride=4), :] = extra[0:8, lanes]
        for q in range(2):
            pltpu.matmul_acc_lhs(accs[q][8], jnp.zeros((48, 256), jnp.bfloat16), load_staged_rhs=0)
            pltpu.matmul_pop(accs[q][8])

    specs = []
    for q in range(2):
        specs += [pltpu.ACC(q)((ROWS, 256), jnp.float32)] * 8 + [pltpu.ACC(q)((48, 256), jnp.float32)]
    pl.run_scoped(run, *specs)


def local_sums(log_weights, bins, states):
    vmem = pl.BlockSpec(memory_space=pltpu.VMEM)
    table = pltpu.VMEM((128, 128), jnp.float32)
    return pl.pallas_call(
        local_kernel,
        out_shape=(
            jax.ShapeDtypeStruct((32, STATE, 128), jnp.float32),
            jax.ShapeDtypeStruct((64, 128), jnp.float32),
        ),
        in_specs=[vmem, vmem, pl.BlockSpec(memory_space=pltpu.HBM)],
        out_specs=(vmem, vmem),
        scratch_shapes=[
            pltpu.VMEM((MARKS, 8, 128), jnp.int32),
            pltpu.VMEM((STATE, COUNT), jnp.bfloat16),
            pltpu.VMEM((256, 128), jnp.bfloat16),
        ] + [table] * 8 + [pltpu.SemaphoreType.DMA],
        compiler_params=pltpu.CompilerParams(vmem_limit_bytes=40 * 1024 * 1024),
        name="local_sums",
    )(bins.reshape(128, 128), log_weights.reshape(128, 128), states)


CHIPS = 16
GROUP = 32


def hops(off):
    return sum(min(part, 4 - part) for part in (off >> 2, off & 3))


ORDER = sorted(range(1, CHIPS), key=lambda off: (-hops(off), off)) + [0]


def lane_sum(row):
    return jnp.broadcast_to(jnp.sum(row, axis=1, keepdims=True), row.shape)


def lane_max(row):
    return jnp.broadcast_to(jnp.max(row, axis=1, keepdims=True), row.shape)


def merge_kernel(whole, sums_ref, tab_ref, weights_ref, cum_ref, means_ref, out_ref,
                 near_ref, near_tab, fac_ref, mate_ref, merged_ref, note_ref, got_ref, got_note,
                 word_ref, words_ref,
                 near_send, near_recv, tab_send, tab_recv, sum_send, sum_recv, note_send, note_recv,
                 word_send, word_recv):
    me = lax.axis_index("dom")
    core = me & 1
    chip = me >> 1
    mate = me ^ 1

    def chip_at(off):
        return ((((chip >> 2) + (off >> 2)) & 3) << 2) | ((chip + (off & 3)) & 3)

    def copy(src, dst, send, recv, target):
        return pltpu.make_async_remote_copy(
            src_ref=src, dst_ref=dst, send_sem=send, recv_sem=recv,
            device_id={"dom": target}, device_id_type=pl.DeviceIdType.MESH)

    barrier = pltpu.get_barrier_semaphore()
    for i in range(1, GROUP):
        pl.semaphore_signal(barrier, 1, device_id={"dom": (me + i) & (GROUP - 1)},
                            device_id_type=pl.DeviceIdType.MESH)
    pl.semaphore_wait(barrier, GROUP - 1)

    tab_copy = copy(tab_ref, near_tab, tab_send, tab_recv, mate)
    tab_copy.start()
    near_copies = []
    for j, off in enumerate(ORDER):
        c = copy(sums_ref.at[2 * chip_at(off) + 1 - core], near_ref.at[j], near_send.at[j],
                 near_recv.at[j], mate)
        c.start()
        near_copies.append(c)

    tab_copy.wait()
    mine = pl.ds(core, CHIPS, stride=2)
    mine_mass = pl.ds(GROUP + core, CHIPS, stride=2)
    top_a, top_b = tab_ref[mine, :], near_tab[mine, :]
    top = jnp.maximum(top_a, top_b)
    fac_a, fac_b = jnp.exp(top_a - top), jnp.exp(top_b - top)
    fac_ref[...] = fac_a
    mate_ref[...] = fac_b
    note_ref[:, 0, :] = top
    note_ref[:, 1, :] = tab_ref[mine_mass, :] * fac_a + near_tab[mine_mass, :] * fac_b

    sum_copies, note_copies = [], []
    for j, off in enumerate(ORDER):
        where = chip_at(off)
        near_copies[j].wait()
        row = pl.ds(where, 1)
        merged_ref[j] = (sums_ref[2 * where + core] * fac_ref[row, :]
                         + near_ref[j] * mate_ref[row, :])
        if off:
            note = copy(note_ref.at[where], got_note.at[j], note_send.at[j], note_recv.at[j],
                        2 * where + core)
            note.start()
            note_copies.append(note)
        if j:
            before = ORDER[j - 1]
            send = copy(merged_ref.at[j - 1], got_ref.at[j - 1], sum_send.at[j - 1], sum_recv.at[j - 1],
                        2 * chip_at(before) + core)
            send.start()
            sum_copies.append(send)

    got_note[CHIPS - 1] = note_ref[chip]
    for c in note_copies:
        c.wait()
    tops = got_note[:, 0, :]
    bin_top = jnp.max(tops, axis=0, keepdims=True)
    factor = jnp.exp(tops - bin_top)
    bin_mass = jnp.sum(got_note[:, 1, :] * factor, axis=0, keepdims=True)
    block_top = lane_max(bin_top)
    word_ref[0:1, :] = block_top
    word_ref[1:2, :] = lane_sum(bin_mass * jnp.exp(bin_top - block_top))
    words_ref[0] = word_ref[...]
    word_copies = []
    for i in range(1, GROUP):
        c = copy(word_ref, words_ref.at[i], word_send.at[i], word_recv.at[i], (me + i) & (GROUP - 1))
        c.start()
        word_copies.append(c)
    for c in word_copies:
        c.wait()
    all_tops, all_masses = words_ref[:, 0, :], words_ref[:, 1, :]
    top_all = jnp.max(all_tops, axis=0, keepdims=True)
    scaled = all_masses * jnp.exp(all_tops - top_all)
    total = jnp.sum(scaled, axis=0, keepdims=True)
    at = lax.broadcasted_iota(jnp.int32, (GROUP, 128), 0)
    lower = (at >= 1) & (at <= me)
    before = jnp.sum(jnp.where(lower, scaled, 0.0), axis=0, keepdims=True)
    run = bin_mass * jnp.exp(bin_top - top_all)
    lane = lax.broadcasted_iota(jnp.int32, (1, 128), 1)
    for level in range(7):
        by = 1 << level
        run = run + jnp.where(lane >= by, pltpu.roll(run, by, 1), 0.0)
    cum_ref[...] = (before + run) / total
    out_ref[...] = jnp.exp(weights_ref[...] - top_all) * (whole / total)

    acc = merged_ref[CHIPS - 1] * factor[CHIPS - 1:CHIPS]
    for j, c in enumerate(sum_copies):
        c.wait()
        acc = acc + got_ref[j] * factor[j:j + 1]
    means_ref[...] = acc / jnp.maximum(bin_mass, 1.0)


def merge(sums, tab, log_weights, whole):
    vmem = pl.BlockSpec(memory_space=pltpu.VMEM)
    dma = pltpu.SemaphoreType.DMA
    f32 = jnp.float32
    return pl.pallas_call(
        functools.partial(merge_kernel, float(whole)),
        out_shape=(
            jax.ShapeDtypeStruct((1, 128), f32),
            jax.ShapeDtypeStruct((STATE, 128), f32),
            jax.ShapeDtypeStruct((128, 128), f32),
        ),
        in_specs=[vmem] * 3,
        out_specs=(vmem,) * 3,
        scratch_shapes=[
            pltpu.VMEM((CHIPS, STATE, 128), f32),
            pltpu.VMEM((2 * GROUP, 128), f32),
            pltpu.VMEM((CHIPS, 128), f32),
            pltpu.VMEM((CHIPS, 128), f32),
            pltpu.VMEM((CHIPS, STATE, 128), f32),
            pltpu.VMEM((CHIPS, 2, 128), f32),
            pltpu.VMEM((CHIPS, STATE, 128), f32),
            pltpu.VMEM((CHIPS, 2, 128), f32),
            pltpu.VMEM((2, 128), f32),
            pltpu.VMEM((GROUP, 2, 128), f32),
            dma((CHIPS,)), dma((CHIPS,)), dma, dma, dma((CHIPS,)), dma((CHIPS,)),
            dma((CHIPS,)), dma((CHIPS,)), dma((GROUP,)), dma((GROUP,)),
        ],
        compiler_params=pltpu.CompilerParams(collective_id=0, has_side_effects=True,
                                             vmem_limit_bytes=24 * 1024 * 1024),
        name="merge",
    )(sums, tab, log_weights.reshape(128, 128))


def body(log_weights, bins, states):
    groups = lax.axis_size("dom")
    sums, tab = local_sums(log_weights, bins, states)
    cumulative, bin_means, particle_weights = merge(sums, tab, log_weights, log_weights.shape[0] * groups)
    return cumulative.reshape(128), bin_means, particle_weights.reshape(COUNT)


def solution(mesh):
    placed = (P(("filt", "dom")), P(("filt", "dom")), P(None, ("filt", "dom")))
    return jax.shard_map(
        body,
        mesh=mesh,
        in_specs=placed,
        out_specs=(P(("filt", "dom")), P(None, ("filt", "dom")), P(("filt", "dom"))),
        check_vma=False,
    )
```

```python
import functools
import jax
import jax.numpy as jnp
from jax import lax
from jax.experimental import pallas as pl
from jax.experimental.pallas import tpu as pltpu
from jax.sharding import PartitionSpec as P

BINS = 4096
FLOOR = -10000.0
COUNT = 16384
STATE = 128
GRAIN = 32
PHASES = (64, 32, 32)
CHIPS = 16
GROUP = 32
CHUNKS = COUNT // 256


def shuffle(x, sub, lane):
    if sub:
        x = jnp.take_along_axis(x, lax.broadcasted_iota(jnp.int32, (8, 128), 0) ^ sub, axis=0,
                                mode="promise_in_bounds")
    if lane:
        x = jnp.take_along_axis(x, lax.broadcasted_iota(jnp.int32, (8, 128), 1) ^ lane, axis=1,
                                mode="promise_in_bounds")
    return x


def is_high(bit):
    if bit < 7:
        return ((lax.broadcasted_iota(jnp.int32, (8, 128), 0) >> (bit - 4)) & 1) == 1
    return ((lax.broadcasted_iota(jnp.int32, (8, 128), 1) >> (bit - 7)) & 1) == 1


def network():
    steps = []
    for k in range(1, 15):
        steps.append((1 << k) - 1)
        for j in range(k - 2, -1, -1):
            steps.append(1 << j)
    return steps


def swap_step(keys, vals, flip, mark_ref, slot):
    top_bit = flip.bit_length() - 1
    vec, sub, lane = flip & 15, (flip >> 4) & 7, flip >> 7
    keys, vals = list(keys), list(vals)
    if not sub and not lane:
        for r in range(16):
            if (r >> top_bit) & 1:
                continue
            q = r ^ vec
            swap = keys[r] > keys[q]
            mark_ref[slot] = swap.astype(jnp.int32)
            slot += 1
            keys[r], keys[q] = jnp.where(swap, keys[q], keys[r]), jnp.where(swap, keys[r], keys[q])
            vals[r], vals[q] = jnp.where(swap, vals[q], vals[r]), jnp.where(swap, vals[r], vals[q])
        return keys, vals, slot
    high = is_high(top_bit)
    other_keys = [shuffle(x, sub, lane) for x in keys]
    other_vals = [shuffle(x, sub, lane) for x in vals]
    out_keys, out_vals = [], []
    for r in range(16):
        q = r ^ vec
        take = (keys[r] > other_keys[q]) ^ high
        mark_ref[slot] = take.astype(jnp.int32)
        slot += 1
        out_keys.append(jnp.where(take, other_keys[q], keys[r]))
        out_vals.append(jnp.where(take, other_vals[q], vals[r]))
    return out_keys, out_vals, slot


def undo_step(vals, flip, mark_ref, slot):
    top_bit = flip.bit_length() - 1
    vec, sub, lane = flip & 15, (flip >> 4) & 7, flip >> 7
    vals = list(vals)
    if not sub and not lane:
        slot -= 8
        at = slot
        for r in range(16):
            if (r >> top_bit) & 1:
                continue
            q = r ^ vec
            swap = mark_ref[at] != 0
            at += 1
            vals[r], vals[q] = jnp.where(swap, vals[q], vals[r]), jnp.where(swap, vals[r], vals[q])
        return vals, slot
    slot -= 16
    others = [shuffle(x, sub, lane) for x in vals]
    return [jnp.where(mark_ref[slot + r] != 0, others[r ^ vec], vals[r]) for r in range(16)], slot


def rotate(x, by, axis):
    size = x.shape[axis]
    at = (lax.broadcasted_iota(jnp.int32, (8, 128), axis) + by) & (size - 1)
    return jnp.take_along_axis(x, at, axis=axis, mode="promise_in_bounds")


def shifted(vecs, by):
    step = abs(by)
    sign = 1 if by > 0 else -1
    if step >= 128:
        return [rotate(x, by // 128, 1) for x in vecs]
    sublane = lax.broadcasted_iota(jnp.int32, (8, 128), 0)

    def carry_sub(x, m):
        moved = rotate(x, m, 0)
        crossed = rotate(moved, sign, 1)
        inside = (sublane + m < 8) if m > 0 else (sublane + m >= 0)
        return jnp.where(inside, moved, crossed)

    if step >= 16:
        return [carry_sub(x, by // 16) for x in vecs]
    out = []
    for r in range(16):
        q = r + by
        out.append(vecs[q] if 0 <= q < 16 else carry_sub(vecs[q % 16], sign))
    return out


def segment_tops(groups, vals):
    for sign in (1, -1):
        for level in range(14):
            by = sign * (1 << level)
            near_groups, near_vals = shifted(groups, by), shifted(vals, by)
            vals = [
                jnp.where(g == ng, jnp.maximum(v, nv), v)
                for g, ng, v, nv in zip(groups, near_groups, vals, near_vals)
            ]
    return vals


def own_tops(bins_ref, weights_ref, mark_ref):
    lane = lax.broadcasted_iota(jnp.int32, (8, 128), 1)
    sublane = lax.broadcasted_iota(jnp.int32, (8, 128), 0)
    keys, vals = [], []
    for r in range(16):
        rows = pl.ds(8 * r, 8)
        keys.append(bins_ref[rows, :] * COUNT + (lane * 128 + sublane * 16 + r))
        vals.append(weights_ref[rows, :])
    slot = 0
    for flip in network():
        keys, vals, slot = swap_step(keys, vals, flip, mark_ref, slot)
    groups = [k >> 14 for k in keys]
    vals = segment_tops(groups, vals)
    for flip in reversed(network()):
        vals, slot = undo_step(vals, flip, mark_ref, slot)
    return vals


MARKS = sum(8 if flip < 16 else 16 for flip in network())


def rows_of(ref, chunk):
    return jnp.concatenate([ref[pl.ds(2 * chunk, 1), :], ref[pl.ds(2 * chunk + 1, 1), :]], axis=1)


def tile_of(row):
    return jnp.broadcast_to(row, (16, 256)).astype(jnp.bfloat16)


def hops(off):
    return sum(min(part, 4 - part) for part in (off >> 2, off & 3))


ORDER = sorted(range(1, CHIPS), key=lambda off: (-hops(off), off))


def lane_sum(row):
    return jnp.broadcast_to(jnp.sum(row, axis=1, keepdims=True), row.shape)


def lane_max(row):
    return jnp.broadcast_to(jnp.max(row, axis=1, keepdims=True), row.shape)


def kernel(whole, bins_hbm, weights_hbm, states_hbm, cum_ref, means_ref, out_ref, refs):
    me = lax.axis_index("dom")
    core = me & 1
    chip = me >> 1
    mate = me ^ 1
    bins_ref, weights_ref, states_ref = refs["bins"], refs["weights"], refs["states"]
    tab_ref, near_tab, note_ref, got_note = refs["tab"], refs["near_tab"], refs["note"], refs["got_note"]
    word_ref, words_ref = refs["word"], refs["words"]

    def chip_at(off):
        return ((((chip >> 2) + (off >> 2)) & 3) << 2) | ((chip + (off & 3)) & 3)

    def copy(src, dst, send, recv, target):
        return pltpu.make_async_remote_copy(
            src_ref=src, dst_ref=dst, send_sem=send, recv_sem=recv,
            device_id={"dom": target}, device_id_type=pl.DeviceIdType.MESH)

    loads = [pltpu.make_async_copy(src, dst, refs["load_sem"].at[i]) for i, (src, dst) in enumerate(
        ((bins_hbm, bins_ref), (weights_hbm, weights_ref), (states_hbm, states_ref)))]
    for load in loads:
        load.start()
    barrier = pltpu.get_barrier_semaphore()
    for i in range(1, GROUP):
        pl.semaphore_signal(barrier, 1, device_id={"dom": (me + i) & (GROUP - 1)},
                            device_id_type=pl.DeviceIdType.MESH)
    loads[0].wait()
    loads[1].wait()

    tops = own_tops(bins_ref, weights_ref, refs["marks"])
    for r in range(16):
        rows = pl.ds(8 * r, 8)
        w, b, top = weights_ref[rows, :], bins_ref[rows, :], tops[r]
        flag = w == top
        refs["scaled"][rows, :] = jnp.where(flag, 1.0, jnp.exp(w - top))
        low = (b & 255).astype(jnp.float32)
        upper = (b & 256) != 0
        refs["key0"][rows, :] = jnp.where(upper, -1.0, low)
        refs["key1"][rows, :] = jnp.where(upper, low, -1.0)
        refs["part"][rows, :] = (b >> 9).astype(jnp.float32)
        t1 = top.astype(jnp.bfloat16).astype(jnp.float32)
        t2 = (top - t1).astype(jnp.bfloat16).astype(jnp.float32)
        t3 = top - t1 - t2
        refs["flag"][rows, :] = jnp.where(flag, 1.0, 0.0)
        refs["t1"][rows, :] = jnp.where(flag, t1, 0.0)
        refs["t2"][rows, :] = jnp.where(flag, t2, 0.0)
        refs["t3"][rows, :] = jnp.where(flag, t3, 0.0)
    iota_ref = refs["iota"]
    iota_ref[...] = lax.broadcasted_iota(jnp.int32, (256, 128), 0).astype(jnp.float32).astype(jnp.bfloat16)
    loads[2].wait()
    pl.semaphore_wait(barrier, GROUP - 1)

    def push(chunk, register):
        scaled = tile_of(rows_of(refs["scaled"], chunk))
        for q in range(2):
            key = tile_of(rows_of(refs["key%d" % q], chunk))
            halves = []
            for side in range(2):
                lanes = slice(128 * side, 128 * side + 128)
                key_full = jnp.concatenate([key[:, lanes]] * 16, axis=0)
                scaled_full = jnp.concatenate([scaled[:, lanes]] * 16, axis=0)
                halves.append(jnp.where(iota_ref[...] == key_full, scaled_full, jnp.bfloat16(0)))
            pltpu.matmul_push_rhs(jnp.concatenate(halves, axis=1), staging_register=register,
                                  mxu_index=q, transpose=True)

    near_copies, tab_copy = [], []

    def send_near(h):
        c = copy(refs["sums%d" % h].at[:, 1 - core], refs["near%d" % h], refs["near_send"].at[h],
                 refs["near_recv"].at[h], mate)
        c.start()
        near_copies.append(c)

    def send_tab():
        c = copy(tab_ref, near_tab, refs["tab_send"], refs["tab_recv"], mate)
        c.start()
        tab_copy.append(c)

    sum_copies, note_copies, word_copies = [], [], []

    def join(h):
        near_copies[h].wait()
        sums, near, merged = refs["sums%d" % h], refs["near%d" % h], refs["merged%d" % h]
        for c in range(CHIPS):
            merged[c] = (sums[c, core] * refs["fac"][c:c + 1, :] + near[c] * refs["mate"][c:c + 1, :])

    def send_sums(h):
        sent = []
        for j, off in enumerate(ORDER):
            where = chip_at(off)
            c = copy(refs["merged%d" % h].at[where], refs["got%d" % h].at[j], refs["sum_send%d" % h].at[j],
                     refs["sum_recv%d" % h].at[j], 2 * where + core)
            c.start()
            sent.append(c)
        sum_copies.append(sent)

    def join_tops():
        tab_copy[0].wait()
        mine = pl.ds(core, CHIPS, stride=2)
        mine_mass = pl.ds(GROUP + core, CHIPS, stride=2)
        top_a, top_b = tab_ref[mine, :], near_tab[mine, :]
        top = jnp.maximum(top_a, top_b)
        fac_a, fac_b = jnp.exp(top_a - top), jnp.exp(top_b - top)
        refs["fac"][...] = fac_a
        refs["mate"][...] = fac_b
        note_ref[:, 0, :] = top
        note_ref[:, 1, :] = tab_ref[mine_mass, :] * fac_a + near_tab[mine_mass, :] * fac_b

    def send_notes():
        for j, off in enumerate(ORDER):
            where = chip_at(off)
            c = copy(note_ref.at[where], got_note.at[j], refs["note_send"].at[j], refs["note_recv"].at[j],
                     2 * where + core)
            c.start()
            note_copies.append(c)
        got_note[CHIPS - 1] = note_ref[chip]

    def join_notes():
        for c in note_copies:
            c.wait()
        tops = got_note[:, 0, :]
        bin_top = jnp.max(tops, axis=0, keepdims=True)
        factor = jnp.exp(tops - bin_top)
        bin_mass = jnp.sum(got_note[:, 1, :] * factor, axis=0, keepdims=True)
        refs["factor"][...] = factor
        refs["owned"][0:1, :] = bin_top
        refs["owned"][1:2, :] = bin_mass
        block_top = lane_max(bin_top)
        word_ref[0:1, :] = block_top
        word_ref[1:2, :] = lane_sum(bin_mass * jnp.exp(bin_top - block_top))
        words_ref[0] = word_ref[...]

    def send_words():
        for i in range(1, GROUP):
            c = copy(word_ref, words_ref.at[i], refs["word_send"].at[i], refs["word_recv"].at[i],
                     (me + i) & (GROUP - 1))
            c.start()
            word_copies.append(c)

    def join_words():
        for c in word_copies:
            c.wait()
        all_tops, all_masses = words_ref[:, 0, :], words_ref[:, 1, :]
        top_all = jnp.max(all_tops, axis=0, keepdims=True)
        scaled = all_masses * jnp.exp(all_tops - top_all)
        total = jnp.sum(scaled, axis=0, keepdims=True)
        at = lax.broadcasted_iota(jnp.int32, (GROUP, 128), 0)
        before = jnp.sum(jnp.where((at >= 1) & (at <= me), scaled, 0.0), axis=0, keepdims=True)
        run = refs["owned"][1:2, :] * jnp.exp(refs["owned"][0:1, :] - top_all)
        lane = lax.broadcasted_iota(jnp.int32, (1, 128), 1)
        for level in range(7):
            by = 1 << level
            run = run + jnp.where(lane >= by, pltpu.roll(run, by, 1), 0.0)
        cum_ref[...] = (before + run) / total
        out_ref[...] = jnp.exp(weights_ref[...] - top_all) * (whole / total)

    def gather_sums(h, start):
        acc = refs["merged%d" % h][chip] * refs["factor"][CHIPS - 1:CHIPS, :]
        for j, c in enumerate(sum_copies[h]):
            c.wait()
            acc = acc + refs["got%d" % h][j] * refs["factor"][j:j + 1, :]
        means_ref[start:start + PHASES[h], :] = acc / jnp.maximum(refs["owned"][1:2, :], 1.0)

    most = max(PHASES) // GRAIN

    def run(*accs):
        size = 8 * most + 1
        accs = (accs[:size], accs[size:])

        def multiply(chunk, register, h):
            part = tile_of(rows_of(refs["part"], chunk))
            cols = pl.ds(pl.multiple_of(chunk * 256, 256), 256)
            first = register
            for g in range(PHASES[h] // GRAIN):
                block = states_ref[pl.ds(sum(PHASES[:h]) + g * GRAIN, GRAIN), cols]
                for p in range(8):
                    mask = jnp.where(part == p, jnp.bfloat16(1), jnp.bfloat16(0))
                    lhs = block * jnp.concatenate([mask] * (GRAIN // 16), axis=0)
                    for q in range(2):
                        pltpu.matmul_acc_lhs(accs[q][g * 8 + p], lhs, load_staged_rhs=first)
                    first = None
            if h == 0:
                row = lax.broadcasted_iota(jnp.int32, (16, 256), 0)
                lower = row < 8
                mine = (row & 7).astype(jnp.float32) == jnp.broadcast_to(rows_of(refs["part"], chunk), (16, 256))
                flag, t1, t2, t3 = (
                    jnp.broadcast_to(rows_of(refs[name], chunk), (16, 256))
                    for name in ("flag", "t1", "t2", "t3")
                )
                groups = (jnp.where(lower, 1.0, flag), jnp.where(lower, t1, t2), jnp.where(lower, t3, 0.0))
                lhs = jnp.concatenate(
                    [jnp.where(mine, g, 0.0).astype(jnp.bfloat16) for g in groups], axis=0)
                for q in range(2):
                    pltpu.matmul_acc_lhs(accs[q][size - 1], lhs)

        def chunks(h, start, stop):
            @pl.loop(start, stop, step=2)
            def _(chunk):
                multiply(chunk, 0, h)
                push(chunk + 1, 1)
                multiply(chunk + 1, 1, h)
                push((chunk + 2) & (CHUNKS - 1), 0)

        def drain(h):
            for g in range(PHASES[h] // GRAIN):
                for p in range(8):
                    for q in range(2):
                        got = pltpu.matmul_pop(accs[q][g * 8 + p])
                        for side in range(2):
                            refs["sums%d" % h][2 * p + q, side, GRAIN * g:GRAIN * g + GRAIN, :] = (
                                got[:, 128 * side:128 * side + 128])

        def drain_tops():
            for q in range(2):
                extra = pltpu.matmul_pop(accs[q][size - 1])
                hits = extra[8:16]
                each = jnp.maximum(hits, 1.0)
                t1, t2, t3 = (
                    (extra[8 * i:8 * i + 8] / each).astype(jnp.bfloat16).astype(jnp.float32)
                    for i in (2, 3, 4)
                )
                top = jnp.where(hits > 0.0, (t1 + t2) + t3, FLOOR)
                for side in range(2):
                    lanes = slice(128 * side, 128 * side + 128)
                    tab_ref[pl.ds(2 * q + side, 8, stride=4), :] = top[:, lanes]
                    tab_ref[pl.ds(GROUP + 2 * q + side, 8, stride=4), :] = extra[0:8, lanes]

        for q in range(2):
            for a in accs[q]:
                pltpu.matmul_pop(a)
        push(0, 0)
        chunks(0, 0, CHUNKS)
        drain_tops()
        drain(0)
        send_tab()
        send_near(0)
        chunks(1, 0, SPLIT[0])
        join_tops()
        join(0)
        send_notes()
        send_sums(0)
        chunks(1, SPLIT[0], CHUNKS)
        drain(1)
        send_near(1)
        chunks(2, 0, SPLIT[1])
        join(1)
        join_notes()
        send_sums(1)
        send_words()
        chunks(2, SPLIT[1], CHUNKS)
        drain(2)
        for q in range(2):
            pltpu.matmul_acc_lhs(accs[q][size - 1], jnp.zeros((48, 256), jnp.bfloat16), load_staged_rhs=0)
            pltpu.matmul_pop(accs[q][size - 1])
        send_near(2)
        join_words()
        join(2)
        gather_sums(0, 0)
        send_sums(2)
        gather_sums(1, PHASES[0])
        gather_sums(2, PHASES[0] + PHASES[1])

    specs = []
    for q in range(2):
        specs += [pltpu.ACC(q)((GRAIN, 256), jnp.float32)] * (8 * most) + [pltpu.ACC(q)((48, 256), jnp.float32)]
    pl.run_scoped(run, *specs)


SPLIT = (32, 32)
VMEM_LIMIT = 67043328


def scratch():
    f32, bf16, dma = jnp.float32, jnp.bfloat16, pltpu.SemaphoreType.DMA
    table = pltpu.VMEM((128, 128), f32)
    shapes = dict(
        bins=pltpu.VMEM((128, 128), jnp.int32), weights=table,
        states=pltpu.VMEM((STATE, COUNT), bf16), marks=pltpu.VMEM((MARKS, 8, 128), jnp.int32),
        iota=pltpu.VMEM((256, 128), bf16), scaled=table, key0=table, key1=table, part=table,
        flag=table, t1=table, t2=table, t3=table,
        tab=pltpu.VMEM((2 * GROUP, 128), f32), near_tab=pltpu.VMEM((2 * GROUP, 128), f32),
        fac=pltpu.VMEM((CHIPS, 128), f32), mate=pltpu.VMEM((CHIPS, 128), f32),
        factor=pltpu.VMEM((CHIPS, 128), f32), owned=pltpu.VMEM((2, 128), f32),
        note=pltpu.VMEM((CHIPS, 2, 128), f32), got_note=pltpu.VMEM((CHIPS, 2, 128), f32),
        word=pltpu.VMEM((2, 128), f32), words=pltpu.VMEM((GROUP, 2, 128), f32),
        load_sem=dma((3,)), near_send=dma((len(PHASES),)), near_recv=dma((len(PHASES),)),
        tab_send=dma, tab_recv=dma, note_send=dma((CHIPS,)), note_recv=dma((CHIPS,)),
        word_send=dma((GROUP,)), word_recv=dma((GROUP,)),
    )
    for h, rows in enumerate(PHASES):
        shapes["sums%d" % h] = pltpu.VMEM((CHIPS, 2, rows, 128), f32)
        for name in ("near", "merged", "got"):
            shapes["%s%d" % (name, h)] = pltpu.VMEM((CHIPS, rows, 128), f32)
        shapes["sum_send%d" % h] = dma((CHIPS,))
        shapes["sum_recv%d" % h] = dma((CHIPS,))
    return shapes


def body(log_weights, bins, states):
    whole = log_weights.shape[0] * lax.axis_size("dom")
    vmem = pl.BlockSpec(memory_space=pltpu.VMEM)
    shapes = scratch()

    def call(*args):
        kernel(float(whole), *args[:6], dict(zip(shapes, args[6:])))

    cumulative, bin_means, particle_weights = pl.pallas_call(
        call,
        out_shape=(
            jax.ShapeDtypeStruct((1, 128), jnp.float32),
            jax.ShapeDtypeStruct((STATE, 128), jnp.float32),
            jax.ShapeDtypeStruct((128, 128), jnp.float32),
        ),
        in_specs=[pl.BlockSpec(memory_space=pltpu.HBM)] * 3,
        out_specs=(vmem,) * 3,
        scratch_shapes=list(shapes.values()),
        compiler_params=pltpu.CompilerParams(collective_id=0, has_side_effects=True,
                                             vmem_limit_bytes=VMEM_LIMIT),
        name="resample",
    )(bins.reshape(128, 128), log_weights.reshape(128, 128), states)
    return cumulative.reshape(128), bin_means, particle_weights.reshape(COUNT)


def solution(mesh):
    placed = (P(("filt", "dom")), P(("filt", "dom")), P(None, ("filt", "dom")))
    return jax.shard_map(
        body,
        mesh=mesh,
        in_specs=placed,
        out_specs=(P(("filt", "dom")), P(None, ("filt", "dom")), P(("filt", "dom"))),
        check_vma=False,
    )
```

```python
import functools
import jax
import jax.numpy as jnp
from jax import lax
from jax.experimental import pallas as pl
from jax.experimental.pallas import tpu as pltpu
from jax.sharding import PartitionSpec as P

BINS = 4096
FLOOR = -10000.0
COUNT = 16384
STATE = 128
GRAIN = 64
PHASES = (2, 2, 2, 1, 1)
JOIN_AT = (24, 24, 24, 40)
UNROLL = 8
CHIPS = 16
GROUP = 32
CHUNKS = COUNT // 256


def shuffle(x, sub, lane):
    if sub:
        x = jnp.take_along_axis(x, lax.broadcasted_iota(jnp.int32, (8, 128), 0) ^ sub, axis=0,
                                mode="promise_in_bounds")
    if lane:
        x = jnp.take_along_axis(x, lax.broadcasted_iota(jnp.int32, (8, 128), 1) ^ lane, axis=1,
                                mode="promise_in_bounds")
    return x


def is_high(bit):
    if bit < 7:
        return ((lax.broadcasted_iota(jnp.int32, (8, 128), 0) >> (bit - 4)) & 1) == 1
    return ((lax.broadcasted_iota(jnp.int32, (8, 128), 1) >> (bit - 7)) & 1) == 1


def network():
    steps = []
    for k in range(1, 15):
        steps.append((1 << k) - 1)
        for j in range(k - 2, -1, -1):
            steps.append(1 << j)
    return steps


def swap_step(keys, vals, flip, mark_ref, slot):
    top_bit = flip.bit_length() - 1
    vec, sub, lane = flip & 15, (flip >> 4) & 7, flip >> 7
    keys, vals = list(keys), list(vals)
    if not sub and not lane:
        for r in range(16):
            if (r >> top_bit) & 1:
                continue
            q = r ^ vec
            swap = keys[r] > keys[q]
            mark_ref[slot] = swap.astype(jnp.int32)
            slot += 1
            keys[r], keys[q] = jnp.where(swap, keys[q], keys[r]), jnp.where(swap, keys[r], keys[q])
            vals[r], vals[q] = jnp.where(swap, vals[q], vals[r]), jnp.where(swap, vals[r], vals[q])
        return keys, vals, slot
    high = is_high(top_bit)
    other_keys = [shuffle(x, sub, lane) for x in keys]
    other_vals = [shuffle(x, sub, lane) for x in vals]
    out_keys, out_vals = [], []
    for r in range(16):
        q = r ^ vec
        take = (keys[r] > other_keys[q]) ^ high
        mark_ref[slot] = take.astype(jnp.int32)
        slot += 1
        out_keys.append(jnp.where(take, other_keys[q], keys[r]))
        out_vals.append(jnp.where(take, other_vals[q], vals[r]))
    return out_keys, out_vals, slot


def undo_step(vals, flip, mark_ref, slot):
    top_bit = flip.bit_length() - 1
    vec, sub, lane = flip & 15, (flip >> 4) & 7, flip >> 7
    vals = list(vals)
    if not sub and not lane:
        slot -= 8
        at = slot
        for r in range(16):
            if (r >> top_bit) & 1:
                continue
            q = r ^ vec
            swap = mark_ref[at] != 0
            at += 1
            vals[r], vals[q] = jnp.where(swap, vals[q], vals[r]), jnp.where(swap, vals[r], vals[q])
        return vals, slot
    slot -= 16
    others = [shuffle(x, sub, lane) for x in vals]
    return [jnp.where(mark_ref[slot + r] != 0, others[r ^ vec], vals[r]) for r in range(16)], slot


def rotate(x, by, axis):
    size = x.shape[axis]
    at = (lax.broadcasted_iota(jnp.int32, (8, 128), axis) + by) & (size - 1)
    return jnp.take_along_axis(x, at, axis=axis, mode="promise_in_bounds")


def shifted(vecs, by):
    step = abs(by)
    sign = 1 if by > 0 else -1
    if step >= 128:
        return [rotate(x, by // 128, 1) for x in vecs]
    sublane = lax.broadcasted_iota(jnp.int32, (8, 128), 0)

    def carry_sub(x, m):
        moved = rotate(x, m, 0)
        crossed = rotate(moved, sign, 1)
        inside = (sublane + m < 8) if m > 0 else (sublane + m >= 0)
        return jnp.where(inside, moved, crossed)

    if step >= 16:
        return [carry_sub(x, by // 16) for x in vecs]
    out = []
    for r in range(16):
        q = r + by
        out.append(vecs[q] if 0 <= q < 16 else carry_sub(vecs[q % 16], sign))
    return out


def segment_tops(groups, vals):
    for sign in (1, -1):
        for level in range(14):
            by = sign * (1 << level)
            near_groups, near_vals = shifted(groups, by), shifted(vals, by)
            vals = [
                jnp.where(g == ng, jnp.maximum(v, nv), v)
                for g, ng, v, nv in zip(groups, near_groups, vals, near_vals)
            ]
    return vals


def own_tops(bins_ref, weights_ref, mark_ref):
    lane = lax.broadcasted_iota(jnp.int32, (8, 128), 1)
    sublane = lax.broadcasted_iota(jnp.int32, (8, 128), 0)
    keys, vals = [], []
    for r in range(16):
        rows = pl.ds(8 * r, 8)
        keys.append(bins_ref[rows, :] * COUNT + (lane * 128 + sublane * 16 + r))
        vals.append(weights_ref[rows, :])
    slot = 0
    for flip in network():
        keys, vals, slot = swap_step(keys, vals, flip, mark_ref, slot)
    groups = [k >> 14 for k in keys]
    vals = segment_tops(groups, vals)
    for flip in reversed(network()):
        vals, slot = undo_step(vals, flip, mark_ref, slot)
    return vals


MARKS = sum(8 if flip < 16 else 16 for flip in network())


def rows_of(ref, chunk):
    return jnp.concatenate([ref[pl.ds(2 * chunk, 1), :], ref[pl.ds(2 * chunk + 1, 1), :]], axis=1)


def tile_of(row):
    return jnp.broadcast_to(row, (16, 256)).astype(jnp.bfloat16)


def hops(off):
    return sum(min(part, 4 - part) for part in (off >> 2, off & 3))


ORDER = sorted(range(1, CHIPS), key=lambda off: (-hops(off), off))


def lane_sum(row):
    return jnp.broadcast_to(jnp.sum(row, axis=1, keepdims=True), row.shape)


def lane_max(row):
    return jnp.broadcast_to(jnp.max(row, axis=1, keepdims=True), row.shape)


def kernel(whole, bins_hbm, weights_hbm, states_hbm, cum_ref, means_ref, out_ref, refs):
    me = lax.axis_index("dom")
    core = me & 1
    chip = me >> 1
    mate = me ^ 1
    bins_ref, weights_ref, states_ref = refs["bins"], refs["weights"], refs["states"]
    tab_ref, near_tab, note_ref, got_note = refs["tab"], refs["near_tab"], refs["note"], refs["got_note"]
    word_ref, words_ref = refs["word"], refs["words"]

    def chip_at(off):
        return ((((chip >> 2) + (off >> 2)) & 3) << 2) | ((chip + (off & 3)) & 3)

    def copy(src, dst, send, recv, target):
        return pltpu.make_async_remote_copy(
            src_ref=src, dst_ref=dst, send_sem=send, recv_sem=recv,
            device_id={"dom": target}, device_id_type=pl.DeviceIdType.MESH)

    loads = [pltpu.make_async_copy(src, dst, refs["load_sem"].at[i]) for i, (src, dst) in enumerate(
        ((bins_hbm, bins_ref), (weights_hbm, weights_ref), (states_hbm, states_ref)))]
    for load in loads:
        load.start()
    barrier = pltpu.get_barrier_semaphore()
    for i in range(1, GROUP):
        pl.semaphore_signal(barrier, 1, device_id={"dom": (me + i) & (GROUP - 1)},
                            device_id_type=pl.DeviceIdType.MESH)
    loads[0].wait()
    loads[1].wait()
    tops = own_tops(bins_ref, weights_ref, refs["marks"])
    for r in range(16):
        rows = pl.ds(8 * r, 8)
        w, b, top = weights_ref[rows, :], bins_ref[rows, :], tops[r]
        flag = w == top
        refs["scaled"][rows, :] = jnp.where(flag, 1.0, jnp.exp(w - top))
        low = (b & 255).astype(jnp.float32)
        upper = (b & 256) != 0
        refs["key0"][rows, :] = jnp.where(upper, -1.0, low)
        refs["key1"][rows, :] = jnp.where(upper, low, -1.0)
        refs["part"][rows, :] = (b >> 9).astype(jnp.float32)
        t1 = top.astype(jnp.bfloat16).astype(jnp.float32)
        t2 = (top - t1).astype(jnp.bfloat16).astype(jnp.float32)
        t3 = top - t1 - t2
        refs["flag"][rows, :] = jnp.where(flag, 1.0, 0.0)
        refs["t1"][rows, :] = jnp.where(flag, t1, 0.0)
        refs["t2"][rows, :] = jnp.where(flag, t2, 0.0)
        refs["t3"][rows, :] = jnp.where(flag, t3, 0.0)
    iota_ref = refs["iota"]
    iota_ref[...] = lax.broadcasted_iota(jnp.int32, (256, 128), 0).astype(jnp.float32).astype(jnp.bfloat16)
    loads[2].wait()

    def push(chunk, register, stored):
        if stored:
            for q in range(2):
                pltpu.matmul_push_rhs(refs["hot"][q, chunk], staging_register=register, mxu_index=q)
            return
        scaled = tile_of(rows_of(refs["scaled"], chunk))
        for q in range(2):
            key = tile_of(rows_of(refs["key%d" % q], chunk))
            halves = []
            for side in range(2):
                lanes = slice(128 * side, 128 * side + 128)
                key_full = jnp.concatenate([key[:, lanes]] * 16, axis=0)
                scaled_full = jnp.concatenate([scaled[:, lanes]] * 16, axis=0)
                half = jnp.where(iota_ref[...] == key_full, scaled_full, jnp.bfloat16(0))
                refs["hot"][q, chunk, lanes, :] = half.T
                halves.append(half)
            pltpu.matmul_push_rhs(jnp.concatenate(halves, axis=1), staging_register=register,
                                  mxu_index=q, transpose=True)

    near_copies, tab_copy = [], []

    def parts_of(h):
        if h < 3:
            row = ((chip >> 2) + (2, 1, 3)[h]) & 3
            return [2 * row, 2 * row + 1]
        return [(chip >> 1) ^ 1] if h == 3 else [chip >> 1]

    def send_near(h):
        c = copy(refs["sums%d" % h].at[:, :, 1 - core], refs["near%d" % h], refs["near_send"].at[h],
                 refs["near_recv"].at[h], mate)
        c.start()
        near_copies.append(c)

    def send_tab():
        c = copy(tab_ref, near_tab, refs["tab_send"], refs["tab_recv"], mate)
        c.start()
        tab_copy.append(c)

    sum_copies, note_copies, word_copies = [], [], []

    def send_sums(h, u, q, where):
        slot = 4 * h + (chip & 3) if h < 3 else (12 + (chip & 1) if h == 3 else 14)
        c = copy(refs["merged%d" % h].at[u, q], refs["got"].at[slot], refs["sum_send"].at[slot_of(h, u, q)],
                 refs["sum_recv"].at[slot], 2 * where + core)
        c.start()
        sum_copies.append(c)

    def slot_of(h, u, q):
        return 4 * h + 2 * u + q if h < 3 else (12 + q if h == 3 else 14)

    def join(h):
        near_copies[h].wait()
        sums, near, merged = refs["sums%d" % h], refs["near%d" % h], refs["merged%d" % h]
        ready = []
        for u, p in enumerate(parts_of(h)):
            for q in ((0, 1) if h < 4 else (1 - (chip & 1), chip & 1)):
                where = 2 * p + q
                row = pl.ds(where, 1)
                merged[u, q] = (sums[u, q, core] * refs["fac"][row, :]
                                + near[u, q] * refs["mate"][row, :])
                ready.append((u, q, where))
                if h < 4 and len(ready) > 1:
                    send_sums(h, *ready[-2])
        send_sums(h, *(ready[-1] if h < 4 else ready[0]))

    def join_tops():
        tab_copy[0].wait()
        mine = pl.ds(core, CHIPS, stride=2)
        mine_mass = pl.ds(GROUP + core, CHIPS, stride=2)
        top_a, top_b = tab_ref[mine, :], near_tab[mine, :]
        top = jnp.maximum(top_a, top_b)
        fac_a, fac_b = jnp.exp(top_a - top), jnp.exp(top_b - top)
        refs["fac"][...] = fac_a
        refs["mate"][...] = fac_b
        note_ref[:, 0, :] = top
        note_ref[:, 1, :] = tab_ref[mine_mass, :] * fac_a + near_tab[mine_mass, :] * fac_b

    def send_notes():
        for j, off in enumerate(ORDER):
            where = chip_at(off)
            c = copy(note_ref.at[where], got_note.at[chip], refs["note_send"].at[j],
                     refs["note_recv"].at[chip], 2 * where + core)
            c.start()
            note_copies.append(c)
        got_note[chip] = note_ref[chip]

    def arrived(dst, recv):
        copy(dst, dst, refs["note_send"].at[0], recv, mate).wait_recv()

    def join_notes():
        for c in note_copies:
            c.wait_send()
        for off in ORDER:
            arrived(got_note.at[chip_at(off)], refs["note_recv"].at[chip_at(off)])
        tops = got_note[:, 0, :]
        bin_top = jnp.max(tops, axis=0, keepdims=True)
        factor = jnp.exp(tops - bin_top)
        bin_mass = jnp.sum(got_note[:, 1, :] * factor, axis=0, keepdims=True)
        refs["factor"][...] = factor
        refs["owned"][0:1, :] = bin_top
        refs["owned"][1:2, :] = bin_mass
        block_top = lane_max(bin_top)
        word_ref[0:1, :] = block_top
        word_ref[1:2, :] = lane_sum(bin_mass * jnp.exp(bin_top - block_top))
        words_ref[0] = word_ref[...]

    def send_words():
        for i in range(1, GROUP):
            c = copy(word_ref, words_ref.at[i], refs["word_send"].at[i], refs["word_recv"].at[i],
                     (me + i) & (GROUP - 1))
            c.start()
            word_copies.append(c)

    def join_words():
        for c in word_copies:
            c.wait()
        all_tops, all_masses = words_ref[:, 0, :], words_ref[:, 1, :]
        top_all = jnp.max(all_tops, axis=0, keepdims=True)
        scaled = all_masses * jnp.exp(all_tops - top_all)
        total = jnp.sum(scaled, axis=0, keepdims=True)
        at = lax.broadcasted_iota(jnp.int32, (GROUP, 128), 0)
        before = jnp.sum(jnp.where((at >= 1) & (at <= me), scaled, 0.0), axis=0, keepdims=True)
        run = refs["owned"][1:2, :] * jnp.exp(refs["owned"][0:1, :] - top_all)
        lane = lax.broadcasted_iota(jnp.int32, (1, 128), 1)
        for level in range(7):
            by = 1 << level
            run = run + jnp.where(lane >= by, pltpu.roll(run, by, 1), 0.0)
        cum_ref[...] = (before + run) / total
        out_ref[...] = jnp.exp(weights_ref[...] - top_all) * (whole / total)

    def gather_sums():
        acc = refs["merged4"][0, chip & 1] * refs["factor"][pl.ds(chip, 1), :]
        for slot in range(15):
            if slot < 12:
                source = ((((chip >> 2) - (2, 1, 3)[slot // 4]) & 3) << 2) | (slot & 3)
            elif slot < 14:
                source = (chip ^ 2) & 14 | (slot & 1)
            else:
                source = chip ^ 1
            arrived(refs["got"].at[slot], refs["sum_recv"].at[slot])
            acc = acc + refs["got"][slot] * refs["factor"][pl.ds(source, 1), :]
        for c in sum_copies:
            c.wait_send()
        means_ref[...] = acc / jnp.maximum(refs["owned"][1:2, :], 1.0)

    grains = STATE // GRAIN

    def run(*accs):
        size = 2 * grains + 1
        accs = (accs[:size], accs[size:])

        def multiply(chunk, register, h):
            part = jnp.broadcast_to(rows_of(refs["part"], chunk), (16, 256))
            cols = pl.ds(pl.multiple_of(chunk * 256, 256), 256)
            first = register
            for u, p in enumerate(parts_of(h)):
                mask = jnp.where(part == p.astype(jnp.float32), 1.0, 0.0).astype(jnp.bfloat16)
                mask = jnp.concatenate([mask] * (GRAIN // 16), axis=0)
                for g in range(grains):
                    lhs = states_ref[pl.ds(g * GRAIN, GRAIN), cols] * mask
                    for q in range(2):
                        pltpu.matmul_acc_lhs(accs[q][u * grains + g], lhs, load_staged_rhs=first)
                    first = None
            if h == 0:
                row = lax.broadcasted_iota(jnp.int32, (16, 256), 0)
                lower = row < 8
                mine = (row & 7).astype(jnp.float32) == part
                flag, t1, t2, t3 = (
                    jnp.broadcast_to(rows_of(refs[name], chunk), (16, 256))
                    for name in ("flag", "t1", "t2", "t3")
                )
                groups = (jnp.where(lower, 1.0, flag), jnp.where(lower, t1, t2), jnp.where(lower, t3, 0.0))
                lhs = jnp.concatenate(
                    [jnp.where(mine, g, 0.0).astype(jnp.bfloat16) for g in groups], axis=0)
                for q in range(2):
                    pltpu.matmul_acc_lhs(accs[q][size - 1], lhs)

        def chunks(h, start, stop):
            @pl.loop(start, stop, step=UNROLL)
            def _(chunk):
                for k in range(UNROLL):
                    multiply(chunk + k, k & 1, h)
                    push((chunk + k + 1) & (CHUNKS - 1), 1 - (k & 1), h > 0)

        def drain(h):
            for u in range(PHASES[h]):
                for g in range(grains):
                    for q in range(2):
                        got = pltpu.matmul_pop(accs[q][u * grains + g])
                        for side in range(2):
                            refs["sums%d" % h][u, q, side, GRAIN * g:GRAIN * g + GRAIN, :] = (
                                got[:, 128 * side:128 * side + 128])

        def drain_tops():
            for q in range(2):
                extra = pltpu.matmul_pop(accs[q][size - 1])
                hits = extra[8:16]
                each = jnp.maximum(hits, 1.0)
                t1, t2, t3 = (
                    (extra[8 * i:8 * i + 8] / each).astype(jnp.bfloat16).astype(jnp.float32)
                    for i in (2, 3, 4)
                )
                top = jnp.where(hits > 0.0, (t1 + t2) + t3, FLOOR)
                for side in range(2):
                    lanes = slice(128 * side, 128 * side + 128)
                    tab_ref[pl.ds(2 * q + side, 8, stride=4), :] = top[:, lanes]
                    tab_ref[pl.ds(GROUP + 2 * q + side, 8, stride=4), :] = extra[0:8, lanes]

        for q in range(2):
            for a in accs[q]:
                pltpu.matmul_pop(a)
        push(0, 0, False)
        chunks(0, 0, CHUNKS)
        drain_tops()
        drain(0)
        for h in range(1, len(PHASES)):
            stop = JOIN_AT[h - 1]
            chunks(h, 0, UNROLL)
            if h == 1:
                pl.semaphore_wait(barrier, GROUP - 1)
                send_tab()
            send_near(h - 1)
            chunks(h, UNROLL, stop)
            if h == 1:
                join_tops()
            if h == 3:
                join_notes()
            join(h - 1)
            if h == 1:
                send_notes()
            if h == 3:
                send_words()
            chunks(h, stop, CHUNKS)
            drain(h)
        for q in range(2):
            pltpu.matmul_acc_lhs(accs[q][size - 1], jnp.zeros((48, 256), jnp.bfloat16), load_staged_rhs=0)
            pltpu.matmul_pop(accs[q][size - 1])
        send_near(len(PHASES) - 1)
        join(len(PHASES) - 1)
        join_words()
        gather_sums()

    specs = []
    for q in range(2):
        specs += [pltpu.ACC(q)((GRAIN, 256), jnp.float32)] * (2 * grains) + [pltpu.ACC(q)((48, 256), jnp.float32)]
    pl.run_scoped(run, *specs)


VMEM_LIMIT = 55040 * 1024


def scratch():
    f32, bf16, dma = jnp.float32, jnp.bfloat16, pltpu.SemaphoreType.DMA
    table = pltpu.VMEM((128, 128), f32)
    shapes = dict(
        bins=pltpu.VMEM((128, 128), jnp.int32), weights=table,
        states=pltpu.VMEM((STATE, COUNT), bf16), hot=pltpu.VMEM((2, CHUNKS, 256, 256), bf16), marks=pltpu.VMEM((MARKS, 8, 128), jnp.int32),
        iota=pltpu.VMEM((256, 128), bf16), scaled=table, key0=table, key1=table, part=table,
        flag=table, t1=table, t2=table, t3=table,
        tab=pltpu.VMEM((2 * GROUP, 128), f32), near_tab=pltpu.VMEM((2 * GROUP, 128), f32),
        fac=pltpu.VMEM((CHIPS, 128), f32), mate=pltpu.VMEM((CHIPS, 128), f32),
        factor=pltpu.VMEM((CHIPS, 128), f32), owned=pltpu.VMEM((2, 128), f32),
        note=pltpu.VMEM((CHIPS, 2, 128), f32), got_note=pltpu.VMEM((CHIPS, 2, 128), f32),
        word=pltpu.VMEM((2, 128), f32), words=pltpu.VMEM((GROUP, 2, 128), f32),
        load_sem=dma((3,)), near_send=dma((len(PHASES),)), near_recv=dma((len(PHASES),)),
        tab_send=dma, tab_recv=dma, note_send=dma((CHIPS,)), note_recv=dma((CHIPS,)),
        word_send=dma((GROUP,)), word_recv=dma((GROUP,)),
    )
    for h, count in enumerate(PHASES):
        shapes["sums%d" % h] = pltpu.VMEM((count, 2, 2, STATE, 128), f32)
        for name in ("near", "merged"):
            shapes["%s%d" % (name, h)] = pltpu.VMEM((count, 2, STATE, 128), f32)
    shapes["got"] = pltpu.VMEM((CHIPS, STATE, 128), f32)
    shapes["sum_send"] = dma((CHIPS,))
    shapes["sum_recv"] = dma((CHIPS,))
    return shapes


def body(log_weights, bins, states):
    whole = log_weights.shape[0] * lax.axis_size("dom")
    vmem = pl.BlockSpec(memory_space=pltpu.VMEM)
    shapes = scratch()

    def call(*args):
        kernel(float(whole), *args[:6], dict(zip(shapes, args[6:])))

    cumulative, bin_means, particle_weights = pl.pallas_call(
        call,
        out_shape=(
            jax.ShapeDtypeStruct((1, 128), jnp.float32),
            jax.ShapeDtypeStruct((STATE, 128), jnp.float32),
            jax.ShapeDtypeStruct((128, 128), jnp.float32),
        ),
        in_specs=[pl.BlockSpec(memory_space=pltpu.HBM)] * 3,
        out_specs=(vmem,) * 3,
        scratch_shapes=list(shapes.values()),
        compiler_params=pltpu.CompilerParams(collective_id=0, has_side_effects=True,
                                             vmem_limit_bytes=VMEM_LIMIT),
        name="resample",
    )(bins.reshape(128, 128), log_weights.reshape(128, 128), states)
    return cumulative.reshape(128), bin_means, particle_weights.reshape(COUNT)


def solution(mesh):
    placed = (P(("filt", "dom")), P(("filt", "dom")), P(None, ("filt", "dom")))
    return jax.shard_map(
        body,
        mesh=mesh,
        in_specs=placed,
        out_specs=(P(("filt", "dom")), P(None, ("filt", "dom")), P(("filt", "dom"))),
        check_vma=False,
    )
```

```python
import functools
import jax
import jax.numpy as jnp
from jax import lax
from jax.experimental import pallas as pl
from jax.experimental.pallas import tpu as pltpu
from jax.sharding import PartitionSpec as P

BINS = 4096
FLOOR = -10000.0
COUNT = 16384
STATE = 128
GRAIN = 64
WIDE = 3
NEAR = (2, 3, 1, 0)
PHASES = WIDE + len(NEAR)
CHIPS = 16
GROUP = 32
CHUNKS = COUNT // 256


def shuffle(x, sub, lane):
    if sub:
        x = jnp.take_along_axis(x, lax.broadcasted_iota(jnp.int32, (8, 128), 0) ^ sub, axis=0,
                                mode="promise_in_bounds")
    if lane:
        x = jnp.take_along_axis(x, lax.broadcasted_iota(jnp.int32, (8, 128), 1) ^ lane, axis=1,
                                mode="promise_in_bounds")
    return x


def is_high(bit):
    if bit < 7:
        return ((lax.broadcasted_iota(jnp.int32, (8, 128), 0) >> (bit - 4)) & 1) == 1
    return ((lax.broadcasted_iota(jnp.int32, (8, 128), 1) >> (bit - 7)) & 1) == 1


def network():
    steps = []
    for k in range(1, 15):
        steps.append((1 << k) - 1)
        for j in range(k - 2, -1, -1):
            steps.append(1 << j)
    return steps


def swap_step(keys, vals, flip, mark_ref, slot):
    top_bit = flip.bit_length() - 1
    vec, sub, lane = flip & 15, (flip >> 4) & 7, flip >> 7
    keys, vals = list(keys), list(vals)
    if not sub and not lane:
        for r in range(16):
            if (r >> top_bit) & 1:
                continue
            q = r ^ vec
            swap = keys[r] > keys[q]
            mark_ref[slot] = swap.astype(jnp.int32)
            slot += 1
            keys[r], keys[q] = jnp.where(swap, keys[q], keys[r]), jnp.where(swap, keys[r], keys[q])
            vals[r], vals[q] = jnp.where(swap, vals[q], vals[r]), jnp.where(swap, vals[r], vals[q])
        return keys, vals, slot
    high = is_high(top_bit)
    other_keys = [shuffle(x, sub, lane) for x in keys]
    other_vals = [shuffle(x, sub, lane) for x in vals]
    out_keys, out_vals = [], []
    for r in range(16):
        q = r ^ vec
        take = (keys[r] > other_keys[q]) ^ high
        mark_ref[slot] = take.astype(jnp.int32)
        slot += 1
        out_keys.append(jnp.where(take, other_keys[q], keys[r]))
        out_vals.append(jnp.where(take, other_vals[q], vals[r]))
    return out_keys, out_vals, slot


def undo_step(vals, flip, mark_ref, slot):
    top_bit = flip.bit_length() - 1
    vec, sub, lane = flip & 15, (flip >> 4) & 7, flip >> 7
    vals = list(vals)
    if not sub and not lane:
        slot -= 8
        at = slot
        for r in range(16):
            if (r >> top_bit) & 1:
                continue
            q = r ^ vec
            swap = mark_ref[at] != 0
            at += 1
            vals[r], vals[q] = jnp.where(swap, vals[q], vals[r]), jnp.where(swap, vals[r], vals[q])
        return vals, slot
    slot -= 16
    others = [shuffle(x, sub, lane) for x in vals]
    return [jnp.where(mark_ref[slot + r] != 0, others[r ^ vec], vals[r]) for r in range(16)], slot


def rotate(x, by, axis):
    size = x.shape[axis]
    at = (lax.broadcasted_iota(jnp.int32, (8, 128), axis) + by) & (size - 1)
    return jnp.take_along_axis(x, at, axis=axis, mode="promise_in_bounds")


def shifted(vecs, by):
    if abs(by) >= 16:
        return [rotate(x, by // 16, 0) for x in vecs]
    return [
        vecs[r + by] if 0 <= r + by < 16 else rotate(vecs[(r + by) % 16], 1 if by > 0 else -1, 0)
        for r in range(16)
    ]


def segment_tops(groups, vals):
    for sign in (1, -1):
        for level in range(7):
            by = sign * (1 << level)
            near_groups, near_vals = shifted(groups, by), shifted(vals, by)
            vals = [
                jnp.where(g == ng, jnp.maximum(v, nv), v)
                for g, ng, v, nv in zip(groups, near_groups, vals, near_vals)
            ]
    first, last = (jnp.broadcast_to(x, (8, 128)) for x in (groups[0][0:1], groups[15][7:8]))
    first_top, last_top = (jnp.broadcast_to(x, (8, 128)) for x in (vals[0][0:1], vals[15][7:8]))
    left, right = last_top, first_top
    for level in range(7):
        by = 1 << level
        left = jnp.where(rotate(last, -by, 1) == last, jnp.maximum(left, rotate(left, -by, 1)), left)
        right = jnp.where(rotate(first, by, 1) == first, jnp.maximum(right, rotate(right, by, 1)), right)
    left = jnp.where(rotate(last, -1, 1) == first, rotate(left, -1, 1), FLOOR)
    right = jnp.where(rotate(first, 1, 1) == last, rotate(right, 1, 1), FLOOR)
    return [
        jnp.maximum(v, jnp.maximum(jnp.where(g == first, left, FLOOR), jnp.where(g == last, right, FLOOR)))
        for g, v in zip(groups, vals)
    ]


def own_tops(bins_ref, weights_ref, mark_ref):
    lane = lax.broadcasted_iota(jnp.int32, (8, 128), 1)
    sublane = lax.broadcasted_iota(jnp.int32, (8, 128), 0)
    keys, vals = [], []
    for r in range(16):
        rows = pl.ds(8 * r, 8)
        keys.append(bins_ref[rows, :] * COUNT + (lane * 128 + sublane * 16 + r))
        vals.append(weights_ref[rows, :])
    slot = 0
    for flip in network():
        keys, vals, slot = swap_step(keys, vals, flip, mark_ref, slot)
    groups = [k >> 14 for k in keys]
    vals = segment_tops(groups, vals)
    for flip in reversed(network()):
        vals, slot = undo_step(vals, flip, mark_ref, slot)
    return vals


MARKS = sum(8 if flip < 16 else 16 for flip in network())


def rows_of(ref, chunk):
    return jnp.concatenate([ref[pl.ds(2 * chunk, 1), :], ref[pl.ds(2 * chunk + 1, 1), :]], axis=1)


def tile_of(row):
    return jnp.broadcast_to(row, (16, 256)).astype(jnp.bfloat16)


def hops(off):
    return sum(min(part, 4 - part) for part in (off >> 2, off & 3))


ORDER = sorted(range(1, CHIPS), key=lambda off: (-hops(off), off))


def lane_sum(row):
    return jnp.broadcast_to(jnp.sum(row, axis=1, keepdims=True), row.shape)


def lane_max(row):
    return jnp.broadcast_to(jnp.max(row, axis=1, keepdims=True), row.shape)


def kernel(whole, bins_hbm, weights_hbm, states_hbm, cum_ref, means_ref, out_ref, refs):
    me = lax.axis_index("dom")
    core = me & 1
    chip = me >> 1
    mate = me ^ 1
    bins_ref, weights_ref, states_ref = refs["bins"], refs["weights"], refs["states"]
    tab_ref, near_tab, note_ref, got_note = refs["tab"], refs["near_tab"], refs["note"], refs["got_note"]
    word_ref, words_ref = refs["word"], refs["words"]

    def chip_at(off):
        return ((((chip >> 2) + (off >> 2)) & 3) << 2) | ((chip + (off & 3)) & 3)

    def copy(src, dst, send, recv, target):
        return pltpu.make_async_remote_copy(
            src_ref=src, dst_ref=dst, send_sem=send, recv_sem=recv,
            device_id={"dom": target}, device_id_type=pl.DeviceIdType.MESH)

    loads = [pltpu.make_async_copy(src, dst, refs["load_sem"].at[i]) for i, (src, dst) in enumerate(
        ((bins_hbm, bins_ref), (weights_hbm, weights_ref), (states_hbm, states_ref)))]
    for load in loads:
        load.start()
    barrier = pltpu.get_barrier_semaphore()
    for i in range(1, GROUP):
        pl.semaphore_signal(barrier, 1, device_id={"dom": (me + i) & (GROUP - 1)},
                            device_id_type=pl.DeviceIdType.MESH)
    loads[0].wait()
    loads[1].wait()
    tops = own_tops(bins_ref, weights_ref, refs["marks"])
    for r in range(16):
        rows = pl.ds(8 * r, 8)
        w, b, top = weights_ref[rows, :], bins_ref[rows, :], tops[r]
        flag = w == top
        refs["scaled"][rows, :] = jnp.where(flag, 1.0, jnp.exp(w - top))
        low = (b & 255).astype(jnp.float32)
        upper = (b & 256) != 0
        refs["key0"][rows, :] = jnp.where(upper, -1.0, low)
        refs["key1"][rows, :] = jnp.where(upper, low, -1.0)
        refs["part"][rows, :] = (b >> 9).astype(jnp.float32)
        t1 = top.astype(jnp.bfloat16).astype(jnp.float32)
        t2 = (top - t1).astype(jnp.bfloat16).astype(jnp.float32)
        t3 = top - t1 - t2
        refs["flag"][rows, :] = jnp.where(flag, 1.0, 0.0)
        refs["t1"][rows, :] = jnp.where(flag, t1, 0.0)
        refs["t2"][rows, :] = jnp.where(flag, t2, 0.0)
        refs["t3"][rows, :] = jnp.where(flag, t3, 0.0)
    iota_ref = refs["iota"]
    iota_ref[...] = lax.broadcasted_iota(jnp.int32, (256, 128), 0).astype(jnp.float32).astype(jnp.bfloat16)
    loads[2].wait()

    def push(h, step, register):
        if h >= WIDE:
            q = target_of(h) & 1
            for m in range(2):
                pltpu.matmul_push_rhs(refs["hot"][q, 2 * step + m], staging_register=register, mxu_index=m)
            return
        if h:
            for q in range(2):
                pltpu.matmul_push_rhs(refs["hot"][q, step], staging_register=register, mxu_index=q)
            return
        chunk = step
        scaled = tile_of(rows_of(refs["scaled"], chunk))
        for q in range(2):
            key = tile_of(rows_of(refs["key%d" % q], chunk))
            halves = []
            for side in range(2):
                lanes = slice(128 * side, 128 * side + 128)
                key_full = jnp.concatenate([key[:, lanes]] * 16, axis=0)
                scaled_full = jnp.concatenate([scaled[:, lanes]] * 16, axis=0)
                half = jnp.where(iota_ref[...] == key_full, scaled_full, jnp.bfloat16(0))
                refs["hot"][q, chunk, lanes, :] = half.T
                halves.append(half)
            pltpu.matmul_push_rhs(jnp.concatenate(halves, axis=1), staging_register=register,
                                  mxu_index=q, transpose=True)

    near_copies, tab_copy = [], []

    row, column = chip >> 2, chip & 3

    def parts_of(h):
        if h == 0:
            away = 2 * ((row + 2) & 3)
            return [away, away + 1]
        return [2 * ((row + by) & 3) + ((column >> 1) ^ (h & 1)) for by in (1, 3)]

    def target_of(h):
        return chip ^ NEAR[h - WIDE]

    def send_near(h):
        sums = refs["sums%d" % h]
        c = copy(sums.at[:, :, 1 - core] if h < WIDE else sums.at[1 - core], refs["near%d" % h],
                 refs["near_send"].at[h], refs["near_recv"].at[h], mate)
        c.start()
        near_copies.append(c)

    def send_tab():
        c = copy(tab_ref, near_tab, refs["tab_send"], refs["tab_recv"], mate)
        c.start()
        tab_copy.append(c)

    sum_copies, note_copies, word_copies = [], [], []

    def send_sums(src, send, slot, where):
        c = copy(src, refs["got"].at[slot], refs["sum_send"].at[send], refs["sum_recv"].at[slot],
                 2 * where + core)
        c.start()
        sum_copies.append(c)

    def join(h):
        near_copies[h].wait()
        sums, near, merged = refs["sums%d" % h], refs["near%d" % h], refs["merged%d" % h]
        if h >= WIDE:
            where = target_of(h)
            at = pl.ds(where, 1)
            merged[...] = sums[core] * refs["fac"][at, :] + near[...] * refs["mate"][at, :]
            if h < PHASES - 1:
                send_sums(merged, 4 * WIDE + h - WIDE, 4 * WIDE + h - WIDE, where)
            return
        ready = []
        for u, p in enumerate(parts_of(h)):
            for q in range(2):
                where = 2 * p + q
                at = pl.ds(where, 1)
                merged[u, q] = (sums[u, q, core] * refs["fac"][at, :]
                                + near[u, q] * refs["mate"][at, :])
                slot = column if h == 0 else 4 * h + 2 * u + (column & 1)
                ready.append((merged.at[u, q], 4 * h + 2 * u + q, slot, where))
                if len(ready) > 1:
                    send_sums(*ready[-2])
        send_sums(*ready[-1])

    def join_tops():
        tab_copy[0].wait()
        mine = pl.ds(core, CHIPS, stride=2)
        mine_mass = pl.ds(GROUP + core, CHIPS, stride=2)
        top_a, top_b = tab_ref[mine, :], near_tab[mine, :]
        top = jnp.maximum(top_a, top_b)
        fac_a, fac_b = jnp.exp(top_a - top), jnp.exp(top_b - top)
        refs["fac"][...] = fac_a
        refs["mate"][...] = fac_b
        note_ref[:, 0, :] = top
        note_ref[:, 1, :] = tab_ref[mine_mass, :] * fac_a + near_tab[mine_mass, :] * fac_b

    def send_notes():
        for j, off in enumerate(ORDER):
            where = chip_at(off)
            c = copy(note_ref.at[where], got_note.at[chip], refs["note_send"].at[j],
                     refs["note_recv"].at[chip], 2 * where + core)
            c.start()
            note_copies.append(c)
        got_note[chip] = note_ref[chip]

    def arrived(dst, recv):
        copy(dst, dst, refs["note_send"].at[0], recv, mate).wait_recv()

    def join_notes():
        for c in note_copies:
            c.wait_send()
        for off in ORDER:
            arrived(got_note.at[chip_at(off)], refs["note_recv"].at[chip_at(off)])
        tops = got_note[:, 0, :]
        bin_top = jnp.max(tops, axis=0, keepdims=True)
        factor = jnp.exp(tops - bin_top)
        bin_mass = jnp.sum(got_note[:, 1, :] * factor, axis=0, keepdims=True)
        refs["factor"][...] = factor
        refs["owned"][0:1, :] = bin_top
        refs["owned"][1:2, :] = bin_mass
        word_ref[0:1, :] = bin_top
        word_ref[1:2, :] = bin_mass
        words_ref[0] = word_ref[...]

    def send_words():
        for i in range(1, GROUP):
            c = copy(word_ref, words_ref.at[i], refs["word_send"].at[i], refs["word_recv"].at[i],
                     (me + i) & (GROUP - 1))
            c.start()
            word_copies.append(c)

    def join_words():
        for c in word_copies:
            c.wait()
        all_tops, all_masses = words_ref[:, 0, :], words_ref[:, 1, :]
        top_all = lane_max(jnp.max(all_tops, axis=0, keepdims=True))
        scaled = all_masses * jnp.exp(all_tops - top_all)
        total = lane_sum(jnp.sum(scaled, axis=0, keepdims=True))
        at = lax.broadcasted_iota(jnp.int32, (GROUP, 128), 0)
        before = lane_sum(jnp.sum(jnp.where((at >= 1) & (at <= me), scaled, 0.0), axis=0, keepdims=True))
        run = refs["owned"][1:2, :] * jnp.exp(refs["owned"][0:1, :] - top_all)
        lane = lax.broadcasted_iota(jnp.int32, (1, 128), 1)
        for level in range(7):
            by = 1 << level
            run = run + jnp.where(lane >= by, pltpu.roll(run, by, 1), 0.0)
        cum_ref[...] = (before + run) / total
        out_ref[...] = jnp.exp(weights_ref[...] - top_all) * (whole / total)

    def gather_sums():
        acc = refs["merged%d" % (PHASES - 1)][...] * refs["factor"][pl.ds(chip, 1), :]
        for slot in range(CHIPS - 1):
            if slot < 4:
                source = (((row - 2) & 3) << 2) | slot
            elif slot < 4 * WIDE:
                source = (((row - (1, 3)[slot // 2 % 2]) & 3) << 2) | (
                    (column ^ (2 if slot < 8 else 0)) & 2) | (slot & 1)
            else:
                source = chip ^ NEAR[slot - 4 * WIDE]
            arrived(refs["got"].at[slot], refs["sum_recv"].at[slot])
            acc = acc + refs["got"][slot] * refs["factor"][pl.ds(source, 1), :]
        for c in sum_copies:
            c.wait_send()
        means_ref[...] = acc / jnp.maximum(refs["owned"][1:2, :], 1.0)

    grains = STATE // GRAIN

    def run(*accs):
        size = 6 * grains + 1
        accs = (accs[:size], accs[size:])

        def factors(chunk, p):
            part = jnp.broadcast_to(rows_of(refs["part"], chunk), (16, 256))
            mask = jnp.where(part == p.astype(jnp.float32), 1.0, 0.0).astype(jnp.bfloat16)
            mask = jnp.concatenate([mask] * (GRAIN // 16), axis=0)
            cols = pl.ds(pl.multiple_of(chunk * 256, 256), 256)
            return [states_ref[pl.ds(g * GRAIN, GRAIN), cols] * mask for g in range(grains)]

        def acc_of(h, q, u, g):
            return accs[q][(2 * (h & 1) + u if h < WIDE else 4 + (h & 1)) * grains + g]

        def multiply(h, chunk, register):
            if h >= WIDE:
                for m in range(2):
                    for g, lhs in enumerate(factors(2 * chunk + m, target_of(h) >> 1)):
                        pltpu.matmul_acc_lhs(acc_of(h, m, 0, g), lhs,
                                             load_staged_rhs=register if g == 0 else None)
                return
            part = jnp.broadcast_to(rows_of(refs["part"], chunk), (16, 256))
            first = register
            for u, p in enumerate(parts_of(h)):
                for g, lhs in enumerate(factors(chunk, p)):
                    for q in range(2):
                        pltpu.matmul_acc_lhs(acc_of(h, q, u, g), lhs, load_staged_rhs=first)
                    first = None
            if h == 0:
                at = lax.broadcasted_iota(jnp.int32, (16, 256), 0)
                lower = at < 8
                mine = (at & 7).astype(jnp.float32) == part
                flag, t1, t2, t3 = (
                    jnp.broadcast_to(rows_of(refs[name], chunk), (16, 256))
                    for name in ("flag", "t1", "t2", "t3")
                )
                groups = (jnp.where(lower, 1.0, flag), jnp.where(lower, t1, t2), jnp.where(lower, t3, 0.0))
                lhs = jnp.concatenate(
                    [jnp.where(mine, g, 0.0).astype(jnp.bfloat16) for g in groups], axis=0)
                for q in range(2):
                    pltpu.matmul_acc_lhs(accs[q][size - 1], lhs)

        def trip(h, step, many, last=False):
            for k in range(many):
                multiply(h, step + k, k & 1)
                if not last or k < many - 1:
                    push(h, step + k + 1, 1 - (k & 1))
                elif h < PHASES - 1:
                    push(h + 1, 0, 0)

        def phase(h, actions):
            end = CHUNKS if h < WIDE else CHUNKS // 2

            def steps(start, stop):
                many = 8 if (stop - start) % 16 else 16
                if stop - start == many:
                    trip(h, start, many)
                elif stop > start:
                    @pl.loop(start, stop, step=many)
                    def _(step):
                        trip(h, step, many)

            trip(h, 0, 8)
            if h:
                drain(h - 1)
            at = 8
            for step in sorted(actions):
                steps(at, step)
                for act in actions[step]:
                    act()
                at = step
            last = 16 if (end - at) % 16 == 0 else 8
            steps(at, end - last)
            trip(h, end - last, last, last=True)

        def drain(h):
            sums = refs["sums%d" % h]
            for u in range(2 if h < WIDE else 1):
                for g in range(grains):
                    rows = slice(GRAIN * g, GRAIN * g + GRAIN)
                    if h >= WIDE:
                        got = pltpu.matmul_pop(acc_of(h, 0, 0, g)) + pltpu.matmul_pop(acc_of(h, 1, 0, g))
                        for side in range(2):
                            sums[side, rows, :] = got[:, 128 * side:128 * side + 128]
                        continue
                    for q in range(2):
                        got = pltpu.matmul_pop(acc_of(h, q, u, g))
                        for side in range(2):
                            sums[u, q, side, rows, :] = got[:, 128 * side:128 * side + 128]
            if h == 0:
                drain_tops()

        def drain_tops():
            for q in range(2):
                extra = pltpu.matmul_pop(accs[q][size - 1])
                hits = extra[8:16]
                each = jnp.maximum(hits, 1.0)
                t1, t2, t3 = (
                    (extra[8 * i:8 * i + 8] / each).astype(jnp.bfloat16).astype(jnp.float32)
                    for i in (2, 3, 4)
                )
                top = jnp.where(hits > 0.0, (t1 + t2) + t3, FLOOR)
                for side in range(2):
                    lanes = slice(128 * side, 128 * side + 128)
                    tab_ref[pl.ds(2 * q + side, 8, stride=4), :] = top[:, lanes]
                    tab_ref[pl.ds(GROUP + 2 * q + side, 8, stride=4), :] = extra[0:8, lanes]

        for q in range(2):
            for a in accs[q]:
                pltpu.matmul_pop(a)
        push(0, 0, 0)
        phase(0, {})

        def greet():
            pl.semaphore_wait(barrier, GROUP - 1)
            send_tab()

        def near(h):
            return functools.partial(send_near, h)

        def meet(h):
            return functools.partial(join, h)

        phase(1, {8: [greet, near(0)], 24: [join_tops, send_notes, meet(0)]})
        phase(2, {8: [near(1)], 24: [meet(1)]})
        phase(3, {8: [near(2)], 16: [join_notes]})
        phase(4, {8: [near(3), send_words], 16: [meet(2)]})
        for h in range(5, PHASES):
            phase(h, {8: [near(h - 1), meet(h - 2)]})
        drain(PHASES - 1)
        join(PHASES - 2)
        send_near(PHASES - 1)
        join_words()
        join(PHASES - 1)
        gather_sums()

    specs = []
    for q in range(2):
        specs += [pltpu.ACC(q)((GRAIN, 256), jnp.float32)] * (6 * grains) + [pltpu.ACC(q)((48, 256), jnp.float32)]
    pl.run_scoped(run, *specs)


VMEM_LIMIT = 55040 * 1024


def scratch():
    f32, bf16, dma = jnp.float32, jnp.bfloat16, pltpu.SemaphoreType.DMA
    table = pltpu.VMEM((128, 128), f32)
    shapes = dict(
        bins=pltpu.VMEM((128, 128), jnp.int32), weights=table,
        states=pltpu.VMEM((STATE, COUNT), bf16), hot=pltpu.VMEM((2, CHUNKS, 256, 256), bf16), marks=pltpu.VMEM((MARKS, 8, 128), jnp.int32),
        iota=pltpu.VMEM((256, 128), bf16), scaled=table, key0=table, key1=table, part=table,
        flag=table, t1=table, t2=table, t3=table,
        tab=pltpu.VMEM((2 * GROUP, 128), f32), near_tab=pltpu.VMEM((2 * GROUP, 128), f32),
        fac=pltpu.VMEM((CHIPS, 128), f32), mate=pltpu.VMEM((CHIPS, 128), f32),
        factor=pltpu.VMEM((CHIPS, 128), f32), owned=pltpu.VMEM((2, 128), f32),
        note=pltpu.VMEM((CHIPS, 2, 128), f32), got_note=pltpu.VMEM((CHIPS, 2, 128), f32),
        word=pltpu.VMEM((2, 128), f32), words=pltpu.VMEM((GROUP, 2, 128), f32),
        load_sem=dma((3,)), near_send=dma((PHASES,)), near_recv=dma((PHASES,)),
        tab_send=dma, tab_recv=dma, note_send=dma((CHIPS,)), note_recv=dma((CHIPS,)),
        word_send=dma((GROUP,)), word_recv=dma((GROUP,)),
    )
    for h in range(PHASES):
        wide = (2, 2) if h < WIDE else ()
        shapes["sums%d" % h] = pltpu.VMEM(wide + (2, STATE, 128), f32)
        for name in ("near", "merged"):
            shapes["%s%d" % (name, h)] = pltpu.VMEM(wide + (STATE, 128), f32)
    shapes["got"] = pltpu.VMEM((CHIPS, STATE, 128), f32)
    shapes["sum_send"] = dma((CHIPS,))
    shapes["sum_recv"] = dma((CHIPS,))
    return shapes


def store_kernel(*refs):
    copies = [pltpu.make_async_copy(refs[i], refs[3 + i], refs[6].at[i]) for i in range(3)]
    for c in copies:
        c.start()
    for c in copies:
        c.wait()


def body(log_weights, bins, states):
    whole = log_weights.shape[0] * lax.axis_size("dom")
    vmem = pl.BlockSpec(memory_space=pltpu.VMEM)
    shapes = scratch()

    def call(*args):
        kernel(float(whole), *args[:6], dict(zip(shapes, args[6:])))

    cumulative, bin_means, particle_weights = pl.pallas_call(
        call,
        out_shape=(
            jax.ShapeDtypeStruct((1, 128), jnp.float32),
            jax.ShapeDtypeStruct((STATE, 128), jnp.float32),
            jax.ShapeDtypeStruct((128, 128), jnp.float32),
        ),
        in_specs=[pl.BlockSpec(memory_space=pltpu.HBM)] * 3,
        out_specs=(vmem,) * 3,
        scratch_shapes=list(shapes.values()),
        compiler_params=pltpu.CompilerParams(collective_id=0, has_side_effects=True,
                                             vmem_limit_bytes=VMEM_LIMIT),
        name="resample",
    )(bins.reshape(128, 128), log_weights.reshape(128, 128), states)
    results = (cumulative, bin_means, particle_weights)
    cumulative, bin_means, particle_weights = pl.pallas_call(
        store_kernel,
        out_shape=[jax.ShapeDtypeStruct(r.shape, r.dtype) for r in results],
        in_specs=[vmem] * 3,
        out_specs=[pl.BlockSpec(memory_space=pltpu.HBM)] * 3,
        scratch_shapes=[pltpu.SemaphoreType.DMA((3,))],
        compiler_params=pltpu.CompilerParams(vmem_limit_bytes=VMEM_LIMIT),
        name="store",
    )(*results)
    return cumulative.reshape(128), bin_means, particle_weights.reshape(COUNT)


def solution(mesh):
    placed = (P(("filt", "dom")), P(("filt", "dom")), P(None, ("filt", "dom")))
    return jax.shard_map(
        body,
        mesh=mesh,
        in_specs=placed,
        out_specs=(P(("filt", "dom")), P(None, ("filt", "dom")), P(("filt", "dom"))),
        check_vma=False,
    )
```

```python
import functools
import jax
import jax.numpy as jnp
from jax import lax
from jax.experimental import pallas as pl
from jax.experimental.pallas import tpu as pltpu
from jax.sharding import PartitionSpec as P

BINS = 4096
FLOOR = -10000.0
COUNT = 16384
STATE = 128
GRAIN = 64
WIDE = 3
TURN_FROM = 11
NEAR = (3, 2, 1, 0)
PHASES = WIDE + len(NEAR)
CHIPS = 16
GROUP = 32
CHUNKS = COUNT // 256


def shuffle(x, sub, lane):
    if sub:
        x = jnp.take_along_axis(x, lax.broadcasted_iota(jnp.int32, (8, 128), 0) ^ sub, axis=0,
                                mode="promise_in_bounds")
    if lane:
        x = jnp.take_along_axis(x, lax.broadcasted_iota(jnp.int32, (8, 128), 1) ^ lane, axis=1,
                                mode="promise_in_bounds")
    return x


def is_high(kind, bit):
    return ((lax.broadcasted_iota(jnp.int32, (8, 128), kind) >> bit) & 1) == 1


def network():
    steps = []
    turned = False
    for k in range(1, 15):
        flips = [((1 << k) - 1, k - 1)] + [(1 << j, j) for j in range(k - 2, -1, -1)]
        for flip, bit in flips:
            turn = k >= TURN_FROM and bit >= 7
            row, lane = flip & 127, flip >> 7
            if turn:
                step = (lane >> 3, lane & 7, (row & 15) << 3 | row >> 4)
                top = (0, bit - 7) if bit < 10 else (2, bit - 10)
            else:
                step = (row & 15, row >> 4, lane)
                top = (2, bit) if bit < 4 else ((0, bit - 4) if bit < 7 else (1, bit - 7))
            steps.append((turn != turned,) + step + top)
            turned = turn
    return steps


def turn_square(vecs):
    square = jnp.concatenate(vecs, axis=0).T
    return [square[8 * r:8 * r + 8] for r in range(16)]


def swap_step(keys, vals, step, mark_ref, slot):
    turn, vec, sub, lane, kind, bit = step
    if turn:
        keys, vals = turn_square(keys), turn_square(vals)
    keys, vals = list(keys), list(vals)
    if not sub and not lane:
        for r in range(16):
            if (r >> bit) & 1:
                continue
            q = r ^ vec
            swap = keys[r] > keys[q]
            mark_ref[slot] = swap.astype(jnp.int32)
            slot += 1
            keys[r], keys[q] = jnp.where(swap, keys[q], keys[r]), jnp.where(swap, keys[r], keys[q])
            vals[r], vals[q] = jnp.where(swap, vals[q], vals[r]), jnp.where(swap, vals[r], vals[q])
        return keys, vals, slot
    other_keys = [shuffle(x, sub, lane) for x in keys]
    other_vals = [shuffle(x, sub, lane) for x in vals]
    out_keys, out_vals = [], []
    for r in range(16):
        q = r ^ vec
        if kind == 2:
            take = (keys[r] < other_keys[q]) if (r >> bit) & 1 else (keys[r] > other_keys[q])
        else:
            take = (keys[r] > other_keys[q]) ^ is_high(kind, bit)
        mark_ref[slot] = take.astype(jnp.int32)
        slot += 1
        out_keys.append(jnp.where(take, other_keys[q], keys[r]))
        out_vals.append(jnp.where(take, other_vals[q], vals[r]))
    return out_keys, out_vals, slot


def undo_step(vals, step, mark_ref, slot):
    turn, vec, sub, lane, kind, bit = step
    vals = list(vals)
    if not sub and not lane:
        slot -= 8
        at = slot
        for r in range(16):
            if (r >> bit) & 1:
                continue
            q = r ^ vec
            swap = mark_ref[at] != 0
            at += 1
            vals[r], vals[q] = jnp.where(swap, vals[q], vals[r]), jnp.where(swap, vals[r], vals[q])
    else:
        slot -= 16
        others = [shuffle(x, sub, lane) for x in vals]
        vals = [jnp.where(mark_ref[slot + r] != 0, others[r ^ vec], vals[r]) for r in range(16)]
    return (turn_square(vals) if turn else vals), slot


def rotate(x, by, axis):
    size = x.shape[axis]
    at = (lax.broadcasted_iota(jnp.int32, (8, 128), axis) + by) & (size - 1)
    return jnp.take_along_axis(x, at, axis=axis, mode="promise_in_bounds")


def shifted(vecs, by):
    if abs(by) >= 16:
        return [rotate(x, by // 16, 0) for x in vecs]
    return [
        vecs[r + by] if 0 <= r + by < 16 else rotate(vecs[(r + by) % 16], 1 if by > 0 else -1, 0)
        for r in range(16)
    ]


def segment_tops(groups, vals):
    for sign in (1, -1):
        for level in range(7):
            by = sign * (1 << level)
            near_groups, near_vals = shifted(groups, by), shifted(vals, by)
            vals = [
                jnp.where(g == ng, jnp.maximum(v, nv), v)
                for g, ng, v, nv in zip(groups, near_groups, vals, near_vals)
            ]
    first, last = (jnp.broadcast_to(x, (8, 128)) for x in (groups[0][0:1], groups[15][7:8]))
    first_top, last_top = (jnp.broadcast_to(x, (8, 128)) for x in (vals[0][0:1], vals[15][7:8]))
    left, right = last_top, first_top
    for level in range(7):
        by = 1 << level
        left = jnp.where(rotate(last, -by, 1) == last, jnp.maximum(left, rotate(left, -by, 1)), left)
        right = jnp.where(rotate(first, by, 1) == first, jnp.maximum(right, rotate(right, by, 1)), right)
    left = jnp.where(rotate(last, -1, 1) == first, rotate(left, -1, 1), FLOOR)
    right = jnp.where(rotate(first, 1, 1) == last, rotate(right, 1, 1), FLOOR)
    return [
        jnp.maximum(v, jnp.maximum(jnp.where(g == first, left, FLOOR), jnp.where(g == last, right, FLOOR)))
        for g, v in zip(groups, vals)
    ]


def own_tops(bins_ref, weights_ref, mark_ref):
    lane = lax.broadcasted_iota(jnp.int32, (8, 128), 1)
    sublane = lax.broadcasted_iota(jnp.int32, (8, 128), 0)
    keys, vals = [], []
    for r in range(16):
        rows = pl.ds(8 * r, 8)
        keys.append(bins_ref[rows, :] * COUNT + (lane * 128 + sublane * 16 + r))
        vals.append(weights_ref[rows, :])
    slot = 0
    for step in network():
        keys, vals, slot = swap_step(keys, vals, step, mark_ref, slot)
    groups = [k >> 14 for k in keys]
    vals = segment_tops(groups, vals)
    for step in reversed(network()):
        vals, slot = undo_step(vals, step, mark_ref, slot)
    return vals


MARKS = sum(16 if step[2] or step[3] else 8 for step in network())


def rows_of(ref, chunk):
    return jnp.concatenate([ref[pl.ds(2 * chunk, 1), :], ref[pl.ds(2 * chunk + 1, 1), :]], axis=1)


def tile_of(row):
    return jnp.broadcast_to(row, (16, 256)).astype(jnp.bfloat16)


def hops(off):
    return sum(min(part, 4 - part) for part in (off >> 2, off & 3))


ORDER = sorted(range(1, CHIPS), key=lambda off: (-hops(off), off))


def lane_sum(row):
    return jnp.broadcast_to(jnp.sum(row, axis=1, keepdims=True), row.shape)


def lane_max(row):
    return jnp.broadcast_to(jnp.max(row, axis=1, keepdims=True), row.shape)


def kernel(whole, bins_hbm, weights_hbm, states_hbm, cum_ref, means_ref, out_ref, refs):
    me = lax.axis_index("dom")
    core = me & 1
    chip = me >> 1
    mate = me ^ 1
    bins_ref, weights_ref, states_ref = refs["bins"], refs["weights"], refs["states"]
    tab_ref, near_tab, note_ref, got_note = refs["tab"], refs["near_tab"], refs["note"], refs["got_note"]
    word_ref, words_ref = refs["word"], refs["words"]

    def chip_at(off):
        return ((((chip >> 2) + (off >> 2)) & 3) << 2) | ((chip + (off & 3)) & 3)

    def copy(src, dst, send, recv, target):
        return pltpu.make_async_remote_copy(
            src_ref=src, dst_ref=dst, send_sem=send, recv_sem=recv,
            device_id={"dom": target}, device_id_type=pl.DeviceIdType.MESH)

    loads = [pltpu.make_async_copy(src, dst, refs["load_sem"].at[i]) for i, (src, dst) in enumerate(
        ((bins_hbm, bins_ref), (weights_hbm, weights_ref), (states_hbm, states_ref)))]
    for load in loads:
        load.start()
    barrier = pltpu.get_barrier_semaphore()
    for i in range(1, GROUP):
        pl.semaphore_signal(barrier, 1, device_id={"dom": (me + i) & (GROUP - 1)},
                            device_id_type=pl.DeviceIdType.MESH)
    loads[0].wait()
    loads[1].wait()
    tops = own_tops(bins_ref, weights_ref, refs["marks"])
    for r in range(16):
        rows = pl.ds(8 * r, 8)
        w, b, top = weights_ref[rows, :], bins_ref[rows, :], tops[r]
        flag = w == top
        refs["scaled"][rows, :] = jnp.where(flag, 1.0, jnp.exp(w - top))
        low = (b & 255).astype(jnp.float32)
        upper = (b & 256) != 0
        refs["key0"][rows, :] = jnp.where(upper, -1.0, low)
        refs["key1"][rows, :] = jnp.where(upper, low, -1.0)
        refs["part"][rows, :] = (b >> 9).astype(jnp.float32)
        t1 = top.astype(jnp.bfloat16).astype(jnp.float32)
        t2 = (top - t1).astype(jnp.bfloat16).astype(jnp.float32)
        t3 = top - t1 - t2
        refs["flag"][rows, :] = jnp.where(flag, 1.0, 0.0)
        refs["t1"][rows, :] = jnp.where(flag, t1, 0.0)
        refs["t2"][rows, :] = jnp.where(flag, t2, 0.0)
        refs["t3"][rows, :] = jnp.where(flag, t3, 0.0)
    iota_ref = refs["iota"]
    iota_ref[...] = lax.broadcasted_iota(jnp.int32, (256, 128), 0).astype(jnp.float32).astype(jnp.bfloat16)
    loads[2].wait()

    def push(h, step, register):
        if h >= WIDE:
            q = target_of(h) & 1
            for m in range(2):
                pltpu.matmul_push_rhs(refs["hot"][q, 2 * step + m], staging_register=register, mxu_index=m)
            return
        if h:
            for q in range(2):
                pltpu.matmul_push_rhs(refs["hot"][q, step], staging_register=register, mxu_index=q)
            return
        chunk = step
        scaled = tile_of(rows_of(refs["scaled"], chunk))
        for q in range(2):
            key = tile_of(rows_of(refs["key%d" % q], chunk))
            halves = []
            for side in range(2):
                lanes = slice(128 * side, 128 * side + 128)
                key_full = jnp.concatenate([key[:, lanes]] * 16, axis=0)
                scaled_full = jnp.concatenate([scaled[:, lanes]] * 16, axis=0)
                half = jnp.where(iota_ref[...] == key_full, scaled_full, jnp.bfloat16(0))
                refs["hot"][q, chunk, lanes, :] = half.T
                halves.append(half)
            pltpu.matmul_push_rhs(jnp.concatenate(halves, axis=1), staging_register=register,
                                  mxu_index=q, transpose=True)

    near_copies, tab_copy = [], []

    row, column = chip >> 2, chip & 3

    def parts_of(h):
        if h == 0:
            away = 2 * ((row + 2) & 3)
            return [away, away + 1]
        return [2 * ((row + by) & 3) + ((column >> 1) ^ (h & 1)) for by in (1, 3)]

    def target_of(h):
        return chip ^ NEAR[h - WIDE]

    def send_near(h):
        sums = refs["sums%d" % h]
        c = copy(sums.at[:, :, 1 - core] if h < WIDE else sums.at[1 - core], refs["near%d" % h],
                 refs["near_send"].at[h], refs["near_recv"].at[h], mate)
        c.start()
        near_copies.append(c)

    def send_tab():
        c = copy(tab_ref, near_tab, refs["tab_send"], refs["tab_recv"], mate)
        c.start()
        tab_copy.append(c)

    sum_copies, note_copies, word_copies = [], [], []

    def send_sums(src, send, slot, where):
        c = copy(src, refs["got"].at[slot], refs["sum_send"].at[send], refs["sum_recv"].at[slot],
                 2 * where + core)
        c.start()
        sum_copies.append(c)

    def join(h):
        near_copies[h].wait()
        sums, near, merged = refs["sums%d" % h], refs["near%d" % h], refs["merged%d" % h]
        if h >= WIDE:
            where = target_of(h)
            at = pl.ds(where, 1)
            merged[...] = sums[core] * refs["fac"][at, :] + near[...] * refs["mate"][at, :]
            if h < PHASES - 1:
                send_sums(merged, 4 * WIDE + h - WIDE, 4 * WIDE + h - WIDE, where)
            return
        ready = []
        for u, p in enumerate(parts_of(h)):
            for q in range(2):
                where = 2 * p + q
                at = pl.ds(where, 1)
                merged[u, q] = (sums[u, q, core] * refs["fac"][at, :]
                                + near[u, q] * refs["mate"][at, :])
                slot = column if h == 0 else 4 * h + 2 * u + (column & 1)
                ready.append((merged.at[u, q], 4 * h + 2 * u + q, slot, where))
                if len(ready) > 1:
                    send_sums(*ready[-2])
        send_sums(*ready[-1])

    def join_tops():
        tab_copy[0].wait()
        mine = pl.ds(core, CHIPS, stride=2)
        mine_mass = pl.ds(GROUP + core, CHIPS, stride=2)
        top_a, top_b = tab_ref[mine, :], near_tab[mine, :]
        top = jnp.maximum(top_a, top_b)
        fac_a, fac_b = jnp.exp(top_a - top), jnp.exp(top_b - top)
        refs["fac"][...] = fac_a
        refs["mate"][...] = fac_b
        note_ref[:, 0, :] = top
        note_ref[:, 1, :] = tab_ref[mine_mass, :] * fac_a + near_tab[mine_mass, :] * fac_b

    def send_notes():
        for j, off in enumerate(ORDER):
            where = chip_at(off)
            c = copy(note_ref.at[where], got_note.at[chip], refs["note_send"].at[j],
                     refs["note_recv"].at[chip], 2 * where + core)
            c.start()
            note_copies.append(c)
        got_note[chip] = note_ref[chip]

    def arrived(dst, recv):
        copy(dst, dst, refs["note_send"].at[0], recv, mate).wait_recv()

    def join_notes():
        for c in note_copies:
            c.wait_send()
        for off in ORDER:
            arrived(got_note.at[chip_at(off)], refs["note_recv"].at[chip_at(off)])
        tops = got_note[:, 0, :]
        bin_top = jnp.max(tops, axis=0, keepdims=True)
        factor = jnp.exp(tops - bin_top)
        bin_mass = jnp.sum(got_note[:, 1, :] * factor, axis=0, keepdims=True)
        refs["factor"][...] = factor
        refs["owned"][0:1, :] = bin_top
        refs["owned"][1:2, :] = bin_mass
        word_ref[0:1, :] = bin_top
        word_ref[1:2, :] = bin_mass
        words_ref[0] = word_ref[...]

    def send_words():
        for i in range(1, GROUP):
            c = copy(word_ref, words_ref.at[i], refs["word_send"].at[i], refs["word_recv"].at[i],
                     (me + i) & (GROUP - 1))
            c.start()
            word_copies.append(c)

    def join_words():
        for c in word_copies:
            c.wait()
        all_tops, all_masses = words_ref[:, 0, :], words_ref[:, 1, :]
        top_all = lane_max(jnp.max(all_tops, axis=0, keepdims=True))
        scaled = all_masses * jnp.exp(all_tops - top_all)
        total = lane_sum(jnp.sum(scaled, axis=0, keepdims=True))
        at = lax.broadcasted_iota(jnp.int32, (GROUP, 128), 0)
        before = lane_sum(jnp.sum(jnp.where((at >= 1) & (at <= me), scaled, 0.0), axis=0, keepdims=True))
        run = refs["owned"][1:2, :] * jnp.exp(refs["owned"][0:1, :] - top_all)
        lane = lax.broadcasted_iota(jnp.int32, (1, 128), 1)
        for level in range(7):
            by = 1 << level
            run = run + jnp.where(lane >= by, pltpu.roll(run, by, 1), 0.0)
        cum_ref[...] = (before + run) / total
        out_ref[...] = jnp.exp(weights_ref[...] - top_all) * (whole / total)

    def gather_sums():
        acc = refs["merged%d" % (PHASES - 1)][...] * refs["factor"][pl.ds(chip, 1), :]
        for slot in range(CHIPS - 1):
            if slot < 4:
                source = (((row - 2) & 3) << 2) | slot
            elif slot < 4 * WIDE:
                source = (((row - (1, 3)[slot // 2 % 2]) & 3) << 2) | (
                    (column ^ (2 if slot < 8 else 0)) & 2) | (slot & 1)
            else:
                source = chip ^ NEAR[slot - 4 * WIDE]
            arrived(refs["got"].at[slot], refs["sum_recv"].at[slot])
            acc = acc + refs["got"][slot] * refs["factor"][pl.ds(source, 1), :]
        for c in sum_copies:
            c.wait_send()
        means_ref[...] = acc / jnp.maximum(refs["owned"][1:2, :], 1.0)

    grains = STATE // GRAIN

    def run(*accs):
        size = 6 * grains + 1
        accs = (accs[:size], accs[size:])

        def factors(chunk, p):
            part = jnp.broadcast_to(rows_of(refs["part"], chunk), (16, 256))
            mask = jnp.where(part == p.astype(jnp.float32), 1.0, 0.0).astype(jnp.bfloat16)
            mask = jnp.concatenate([mask] * (GRAIN // 16), axis=0)
            cols = pl.ds(pl.multiple_of(chunk * 256, 256), 256)
            return [states_ref[pl.ds(g * GRAIN, GRAIN), cols] * mask for g in range(grains)]

        def acc_of(h, q, u, g):
            return accs[q][(2 * (h & 1) + u if h < WIDE else 4 + (h & 1)) * grains + g]

        def multiply(h, chunk, register):
            if h >= WIDE:
                for m in range(2):
                    for g, lhs in enumerate(factors(2 * chunk + m, target_of(h) >> 1)):
                        pltpu.matmul_acc_lhs(acc_of(h, m, 0, g), lhs,
                                             load_staged_rhs=register if g == 0 else None)
                return
            part = jnp.broadcast_to(rows_of(refs["part"], chunk), (16, 256))
            first = register
            for u, p in enumerate(parts_of(h)):
                for g, lhs in enumerate(factors(chunk, p)):
                    for q in range(2):
                        pltpu.matmul_acc_lhs(acc_of(h, q, u, g), lhs, load_staged_rhs=first)
                    first = None
            if h == 0:
                at = lax.broadcasted_iota(jnp.int32, (16, 256), 0)
                lower = at < 8
                mine = (at & 7).astype(jnp.float32) == part
                flag, t1, t2, t3 = (
                    jnp.broadcast_to(rows_of(refs[name], chunk), (16, 256))
                    for name in ("flag", "t1", "t2", "t3")
                )
                groups = (jnp.where(lower, 1.0, flag), jnp.where(lower, t1, t2), jnp.where(lower, t3, 0.0))
                lhs = jnp.concatenate(
                    [jnp.where(mine, g, 0.0).astype(jnp.bfloat16) for g in groups], axis=0)
                for q in range(2):
                    pltpu.matmul_acc_lhs(accs[q][size - 1], lhs)

        def trip(h, step, many, last=False):
            for k in range(many):
                multiply(h, step + k, k & 1)
                if not last or k < many - 1:
                    push(h, step + k + 1, 1 - (k & 1))
                elif h < PHASES - 1:
                    push(h + 1, 0, 0)

        def phase(h, actions):
            end = CHUNKS if h < WIDE else CHUNKS // 2

            def steps(start, stop):
                many = 8 if (stop - start) % 16 else 16
                if stop - start == many:
                    trip(h, start, many)
                elif stop > start:
                    @pl.loop(start, stop, step=many)
                    def _(step):
                        trip(h, step, many)

            trip(h, 0, 8)
            if h:
                drain(h - 1)
            at = 8
            for step in sorted(actions):
                steps(at, step)
                for act in actions[step]:
                    act()
                at = step
            last = 16 if (end - at) % 16 == 0 else 8
            steps(at, end - last)
            trip(h, end - last, last, last=True)

        def drain(h):
            sums = refs["sums%d" % h]
            for u in range(2 if h < WIDE else 1):
                for g in range(grains):
                    rows = slice(GRAIN * g, GRAIN * g + GRAIN)
                    if h >= WIDE:
                        got = pltpu.matmul_pop(acc_of(h, 0, 0, g)) + pltpu.matmul_pop(acc_of(h, 1, 0, g))
                        for side in range(2):
                            sums[side, rows, :] = got[:, 128 * side:128 * side + 128]
                        continue
                    for q in range(2):
                        got = pltpu.matmul_pop(acc_of(h, q, u, g))
                        for side in range(2):
                            sums[u, q, side, rows, :] = got[:, 128 * side:128 * side + 128]
            if h == 0:
                drain_tops()

        def drain_tops():
            for q in range(2):
                extra = pltpu.matmul_pop(accs[q][size - 1])
                hits = extra[8:16]
                each = jnp.maximum(hits, 1.0)
                t1, t2, t3 = (
                    (extra[8 * i:8 * i + 8] / each).astype(jnp.bfloat16).astype(jnp.float32)
                    for i in (2, 3, 4)
                )
                top = jnp.where(hits > 0.0, (t1 + t2) + t3, FLOOR)
                for side in range(2):
                    lanes = slice(128 * side, 128 * side + 128)
                    tab_ref[pl.ds(2 * q + side, 8, stride=4), :] = top[:, lanes]
                    tab_ref[pl.ds(GROUP + 2 * q + side, 8, stride=4), :] = extra[0:8, lanes]

        for q in range(2):
            for a in accs[q]:
                pltpu.matmul_pop(a)
        push(0, 0, 0)
        phase(0, {})

        def greet():
            pl.semaphore_wait(barrier, GROUP - 1)
            send_tab()

        def near(h):
            return functools.partial(send_near, h)

        def meet(h):
            return functools.partial(join, h)

        phase(1, {8: [greet, near(0)], 24: [join_tops, send_notes, meet(0)]})
        phase(2, {8: [near(1)], 24: [meet(1)]})
        phase(3, {8: [near(2), join_notes], 16: [send_words]})
        phase(4, {8: [near(3), meet(2)]})
        for h in range(5, PHASES):
            phase(h, {8: [near(h - 1), meet(h - 2)]})
        drain(PHASES - 1)
        join(PHASES - 2)
        send_near(PHASES - 1)
        join_words()
        join(PHASES - 1)
        gather_sums()

    specs = []
    for q in range(2):
        specs += [pltpu.ACC(q)((GRAIN, 256), jnp.float32)] * (6 * grains) + [pltpu.ACC(q)((48, 256), jnp.float32)]
    pl.run_scoped(run, *specs)


VMEM_LIMIT = 55040 * 1024


def scratch():
    f32, bf16, dma = jnp.float32, jnp.bfloat16, pltpu.SemaphoreType.DMA
    table = pltpu.VMEM((128, 128), f32)
    shapes = dict(
        bins=pltpu.VMEM((128, 128), jnp.int32), weights=table,
        states=pltpu.VMEM((STATE, COUNT), bf16), hot=pltpu.VMEM((2, CHUNKS, 256, 256), bf16), marks=pltpu.VMEM((MARKS, 8, 128), jnp.int32),
        iota=pltpu.VMEM((256, 128), bf16), scaled=table, key0=table, key1=table, part=table,
        flag=table, t1=table, t2=table, t3=table,
        tab=pltpu.VMEM((2 * GROUP, 128), f32), near_tab=pltpu.VMEM((2 * GROUP, 128), f32),
        fac=pltpu.VMEM((CHIPS, 128), f32), mate=pltpu.VMEM((CHIPS, 128), f32),
        factor=pltpu.VMEM((CHIPS, 128), f32), owned=pltpu.VMEM((2, 128), f32),
        note=pltpu.VMEM((CHIPS, 2, 128), f32), got_note=pltpu.VMEM((CHIPS, 2, 128), f32),
        word=pltpu.VMEM((2, 128), f32), words=pltpu.VMEM((GROUP, 2, 128), f32),
        load_sem=dma((3,)), near_send=dma((PHASES,)), near_recv=dma((PHASES,)),
        tab_send=dma, tab_recv=dma, note_send=dma((CHIPS,)), note_recv=dma((CHIPS,)),
        word_send=dma((GROUP,)), word_recv=dma((GROUP,)),
    )
    for h in range(PHASES):
        wide = (2, 2) if h < WIDE else ()
        shapes["sums%d" % h] = pltpu.VMEM(wide + (2, STATE, 128), f32)
        for name in ("near", "merged"):
            shapes["%s%d" % (name, h)] = pltpu.VMEM(wide + (STATE, 128), f32)
    shapes["got"] = pltpu.VMEM((CHIPS, STATE, 128), f32)
    shapes["sum_send"] = dma((CHIPS,))
    shapes["sum_recv"] = dma((CHIPS,))
    return shapes


def store_kernel(*refs):
    copies = [pltpu.make_async_copy(refs[i], refs[3 + i], refs[6].at[i]) for i in range(3)]
    for c in copies:
        c.start()
    for c in copies:
        c.wait()


def body(log_weights, bins, states):
    whole = log_weights.shape[0] * lax.axis_size("dom")
    vmem = pl.BlockSpec(memory_space=pltpu.VMEM)
    shapes = scratch()

    def call(*args):
        kernel(float(whole), *args[:6], dict(zip(shapes, args[6:])))

    cumulative, bin_means, particle_weights = pl.pallas_call(
        call,
        out_shape=(
            jax.ShapeDtypeStruct((1, 128), jnp.float32),
            jax.ShapeDtypeStruct((STATE, 128), jnp.float32),
            jax.ShapeDtypeStruct((128, 128), jnp.float32),
        ),
        in_specs=[pl.BlockSpec(memory_space=pltpu.HBM)] * 3,
        out_specs=(vmem,) * 3,
        scratch_shapes=list(shapes.values()),
        compiler_params=pltpu.CompilerParams(collective_id=0, has_side_effects=True,
                                             vmem_limit_bytes=VMEM_LIMIT),
        name="resample",
    )(bins.reshape(128, 128), log_weights.reshape(128, 128), states)
    results = (cumulative, bin_means, particle_weights)
    cumulative, bin_means, particle_weights = pl.pallas_call(
        store_kernel,
        out_shape=[jax.ShapeDtypeStruct(r.shape, r.dtype) for r in results],
        in_specs=[vmem] * 3,
        out_specs=[pl.BlockSpec(memory_space=pltpu.HBM)] * 3,
        scratch_shapes=[pltpu.SemaphoreType.DMA((3,))],
        compiler_params=pltpu.CompilerParams(vmem_limit_bytes=VMEM_LIMIT),
        name="store",
    )(*results)
    return cumulative.reshape(128), bin_means, particle_weights.reshape(COUNT)


def solution(mesh):
    placed = (P(("filt", "dom")), P(("filt", "dom")), P(None, ("filt", "dom")))
    return jax.shard_map(
        body,
        mesh=mesh,
        in_specs=placed,
        out_specs=(P(("filt", "dom")), P(None, ("filt", "dom")), P(("filt", "dom"))),
        check_vma=False,
    )
```
